256 devices in a mesh: gx: 8 (over z), gy: 4 (over x), gz: 8 (over y, core).
Axes of the slice: x: 4, y: 4, z: 8, core: 2. Of those that a mesh axis runs over, the one named last changes fastest.
Arguments:
- source: float32 [64, 128, 1024], P('gx', 'gy', 'gz'), may hold values from 0.05 to 1
- target: float32 [64, 128, 1024], P('gx', 'gy', 'gz'), may hold values from 0.05 to 1
- kernel_half: float32 [5], replicated, may hold values from 0.05 to 1
- smooth_half: float32 [9], replicated, may hold values from 0.1 to 1
Outputs:
- displacement: float32 [3, 64, 128, 1024], P(None, 'gx', 'gy', 'gz')
- mismatch: float32 [6], replicated
The draws below stay inside these ranges and needn't reach their ends.
All inputs are finite; a program needn't handle non-finite values.
Results may differ from the reference program's by a relative error of at most 0.0001.
Values sent between devices are 32-bit elements; how exact they have to be, the bound alone decides.
A program may use at most 64 MiB of HBM per device.

```python
import math
import jax
import jax.numpy as jnp
from jax import lax

ITERS = 6
RADIUS = 4
SMOOTH = 8
NX = 64
NY = 128
NZ = 1024


def level_of(own_key, extent, split, least, largest):
    def one(axis_at, shards_of):
        steps = jax.random.uniform(jax.random.fold_in(jax.random.fold_in(own_key, 6), axis_at), (shards_of,), jnp.float32, least / len(split), largest / len(split))
        return jnp.repeat(jnp.exp(steps), extent[axis_at] // shards_of).reshape((-1,) + (1,) * (len(extent) - axis_at - 1))

    factor_of = one(*split[0])
    for cut in split[1:]:
        factor_of = factor_of * one(*cut)
    return factor_of


def setup_inputs(seed: int = 0) -> dict:
    splits = jax.random.split(jax.random.key(seed), 5)
    return {
        "source": jnp.clip(jnp.exp(math.log(1.0) - 2.9957323 * jax.random.uniform(splits[0], (NX, NY, NZ), jnp.float32) ** level_of(splits[0], (NX, NY, NZ), ((0, 8), (1, 4), (2, 8)), -0.2, 0.2)), 0.05, 1.0),
        "target": jnp.clip(jnp.exp(math.log(1.0) - 2.9957323 * jax.random.uniform(splits[1], (NX, NY, NZ), jnp.float32) ** level_of(splits[1], (NX, NY, NZ), ((0, 8), (1, 4), (2, 8)), -0.2, 0.2)), 0.05, 1.0),
        "kernel_half": jnp.clip(jnp.exp(jax.random.uniform(splits[2], (RADIUS + 1,), jnp.float32, math.log(0.05), math.log(1.0))), 0.05, 1.0),
        "smooth_half": jnp.clip(jnp.exp(jax.random.uniform(splits[3], (SMOOTH + 1,), jnp.float32, math.log(0.1), math.log(1.0))), 0.1, 1.0),
    }


def full_taps(half):
    return jnp.concatenate([half[:0:-1], half])


def along(padded, taps, axis, count):
    width = taps.shape[0]
    total = taps[0] * lax.slice_in_dim(padded, 0, count, axis=axis)
    for j in range(1, width):
        total = total + taps[j] * lax.slice_in_dim(padded, j, j + count, axis=axis)
    return total


def kernel_apply(field, taps):
    radius = (taps.shape[0] - 1) // 2
    padded = jnp.pad(field, radius)
    padded = along(padded, taps, 0, NX)
    padded = along(padded, taps, 1, NY)
    return along(padded, taps, 2, NZ)


def reference(source, target, kernel_half, smooth_half):
    kern = full_taps(kernel_half)
    offsets = jnp.arange(-RADIUS, RADIUS + 1).astype(jnp.float32)
    slope = offsets * kern
    norm_total = smooth_half[0] + 2.0 * jnp.sum(smooth_half[1:])
    smooth = full_taps(smooth_half) / norm_total
    cells = float(NX * NY * NZ)
    first = source * (cells / jnp.sum(source))
    second = target * (cells / jnp.sum(target))
    scaling_v = jnp.ones_like(source)
    errors = []
    for step in range(ITERS):
        kv = kernel_apply(scaling_v, kern)
        scaling_u = first / kv
        ku = kernel_apply(scaling_u, kern)
        errors.append(jnp.sum(jnp.abs(scaling_v * ku - second)) / cells)
        scaling_v = second / ku
    padded = jnp.pad(scaling_v, RADIUS)
    pass_k = along(padded, kern, 0, NX)
    pass_g = along(padded, slope, 0, NX)
    kk = along(pass_k, kern, 1, NY)
    kg = along(pass_k, slope, 1, NY)
    gk = along(pass_g, kern, 1, NY)
    kvol = along(kk, kern, 2, NZ)
    znum = along(kk, slope, 2, NZ)
    ynum = along(kg, kern, 2, NZ)
    xnum = along(gk, kern, 2, NZ)
    raw = jnp.stack([xnum, ynum, znum]) / kvol
    padded = jnp.pad(raw, ((0, 0), (SMOOTH, SMOOTH), (SMOOTH, SMOOTH), (SMOOTH, SMOOTH)))
    padded = along(padded, smooth, 1, NX)
    padded = along(padded, smooth, 2, NY)
    displacement = along(padded, smooth, 3, NZ)
    return displacement, jnp.stack(errors)
```

```python
import functools

import jax
import jax.numpy as jnp
from jax import lax
from jax.experimental import pallas as pl
from jax.experimental.pallas import tpu as pltpu
from jax.sharding import PartitionSpec as P

ITERS = 6
R = 4
S = 8
BX, BY, BZ = 8, 32, 128
TY = BY // 8
MESH = pl.DeviceIdType.MESH
F32 = jnp.float32

DIRS = sorted(
    [
        (dx, dy, dz)
        for dx in (-1, 0, 1)
        for dy in (-1, 0, 1)
        for dz in (-1, 0, 1)
        if (dx, dy, dz) != (0, 0, 0)
    ],
    key=lambda d: (-sum(abs(c) for c in d), abs(d[0]), abs(d[1]), d),
)
YZ = [d for d in DIRS if d[0] == 0]


def kernel(
    sizes,
    src_hbm, tgt_hbm, kern, smo,
    disp_hbm, mis,
    a_ref, b_ref, f, zp, zb, t, tz, w, tots, totb, out,
    xb, yb, pz, zs, t2, tz2,
    send, recv, xsend, xrecv, ysend, yrecv, lsend, lrecv, loc,
):
    nx, ny, nz = sizes
    cells = float(nx * ny * nz * BX * BY * BZ)
    mx, my, mz = lax.axis_index("gx"), lax.axis_index("gy"), lax.axis_index("gz")
    pos = {"gx": (mx, nx), "gy": (my, ny), "gz": (mz, nz)}
    lane = lax.broadcasted_iota(jnp.int32, (8, BZ), 1)
    sub = lax.broadcasted_iota(jnp.int32, (8, BZ), 0)
    zero = jnp.zeros((8, BZ), F32)

    loads = [
        pltpu.make_async_copy(src_hbm, a_ref, loc.at[0]),
        pltpu.make_async_copy(tgt_hbm, b_ref, loc.at[1]),
    ]
    for c in loads:
        c.start()

    def inside(m, n, d):
        if d == 0:
            return None
        return m + d < n if d > 0 else m + d >= 0

    conds = [{d: inside(m, n, d) for d in (-1, 0, 1)} for m, n in pos.values()]

    def has(d):
        c = [conds[i][d[i]] for i in range(3) if d[i]]
        return functools.reduce(jnp.logical_and, c)

    def peer(d):
        ids = {}
        for axis, step in zip(pos, d):
            if step:
                ids[axis] = pos[axis][0] + step
        return ids

    def neg(d):
        return tuple(-c for c in d)

    for p in range(2):
        for i in range(2 * R + BX):
            for j in range(TY + 2):
                f[p, i, pl.ds(8 * j, 8), :] = zero
        for q in range(2):
            for e in range(3):
                for j in range(4):
                    zb[p, q, e, pl.ds(8 * j, 8), :] = zero

    barrier = pltpu.get_barrier_semaphore()
    expected = sum(n - 1 for _, n in pos.values())
    for axis, (m, n) in pos.items():
        for j in range(1, n):
            pl.semaphore_signal(
                barrier, 1, device_id={axis: lax.rem(m + j, n)}, device_id_type=MESH
            )
    for d in DIRS:
        if sum(abs(c) for c in d) > 1:
            there = has(d)
            expected = expected + jnp.where(there, 1, 0)

            @pl.when(there)
            def _():
                pl.semaphore_signal(barrier, 1, device_id=peer(d), device_id_type=MESH)

    k = [kern[i] for i in range(R + 1)]
    norm = smo[0]
    tail = smo[1]
    for i in range(2, S + 1):
        tail = tail + smo[i]
    norm = jnp.full((8, BZ), norm + 2.0 * tail, F32)
    s = [jnp.full((8, BZ), smo[i], F32) / norm for i in range(S + 1)]

    for c in range(3):
        for i in range(BX):
            for j in range(TY):
                xb[c, i, pl.ds(8 * j, 8), :] = zero
                xb[c, 2 * BX + i, pl.ds(8 * j, 8), :] = zero
            for j in (0, TY + 1):
                yb[c, i, pl.ds(8 * j, 8), :] = zero
        for q in range(2):
            for j in range(TY + 2):
                zs[c, q, pl.ds(8 * j, 8), :] = zero

    def copy(p, d):
        i = DIRS.index(d)
        dx, dy, dz = d
        if dz == 0:
            xs = {1: pl.ds(BX, R), -1: pl.ds(R, R), 0: pl.ds(R, BX)}[dx]
            xd = {1: pl.ds(0, R), -1: pl.ds(R + BX, R), 0: pl.ds(R, BX)}[dx]
            ys = {1: pl.ds(BY, 8), -1: pl.ds(8, 8), 0: pl.ds(8, BY)}[dy]
            yd = {1: pl.ds(0, 8), -1: pl.ds(BY + 8, 8), 0: pl.ds(8, BY)}[dy]
            source, target = f.at[p, xs, ys], f.at[p, xd, yd]
        else:
            side = 0 if dz > 0 else 1
            rows = {1: pl.ds(8, 8), -1: pl.ds(0, 8), 0: pl.ds(0, 16)}[dy]
            lands = {1: pl.ds(0, 8), -1: pl.ds(24, 8), 0: pl.ds(8, 16)}[dy]
            source, target = zp.at[p, rows], zb.at[p, side, 1 - dx, lands]
        return pltpu.make_async_remote_copy(
            src_ref=source, dst_ref=target, send_sem=send.at[p, i],
            recv_sem=recv.at[p, i], device_id=peer(d), device_id_type=MESH,
        )

    def start(p):
        for d in DIRS:
            @pl.when(has(d))
            def _():
                copy(p, d).start()

    def sent(p):
        for d in DIRS:
            @pl.when(has(d))
            def _():
                copy(p, d).wait_send()

    def arrived(p, dirs):
        for d in dirs:
            @pl.when(has(neg(d)))
            def _():
                copy(p, d).wait_recv()

    def line(axis, q, go):
        m, n = pos[axis]
        base = {"gx": 0, "gy": nx - 1, "gz": nx + ny - 2}[axis]
        for j in range(1, n):
            c = pltpu.make_async_remote_copy(
                src_ref=tots.at[q, "xyz".index(axis[1])], dst_ref=totb.at[q, base + j - 1],
                send_sem=lsend.at[q, base + j - 1], recv_sem=lrecv.at[q, base + j - 1],
                device_id={axis: lax.rem(m + j, n)}, device_id_type=MESH,
            )
            if go:
                c.start()
            else:
                c.wait()

    def line_end(axis, q):
        line(axis, q, False)
        n = pos[axis][1]
        a = "xyz".index(axis[1])
        base = {"gx": 0, "gy": nx - 1, "gz": nx + ny - 2}[axis]
        v = tots[q, a]
        for j in range(1, n):
            v = v + totb[q, base + j - 1]
        tots[q, a + 1] = v

    def symmetric(taps, at):
        acc = taps[0] * at(0)
        for d in range(1, len(taps)):
            acc = acc + taps[d] * (at(d) + at(-d))
        return acc

    def slope(taps, at):
        acc = None
        for d in range(1, len(taps)):
            term = (float(d) * taps[d]) * (at(d) - at(-d))
            acc = term if acc is None else acc + term
        return acc

    def roll(v, by):
        by = by % BZ
        return v if by == 0 else pltpu.roll(v, by, 1)

    def along_z(own, halo, taps, passes):
        n = len(taps)
        shifted = {0: own}
        for d in range(1, n):
            shifted[d] = roll(jnp.where(lane < d, halo, own), -d)
            shifted[-d] = roll(jnp.where(lane >= BZ - d, halo, own), d)
        return [q(taps, lambda d: shifted[d]) for q in passes]

    def packed_in(p):
        left = (lane % 8) < R
        tiles = []
        for e in range(4):
            rows = pl.ds(8 * e, 8)
            face = jnp.where(left, zb[p, 0, 1, rows, :], zb[p, 1, 1, rows, :])
            low = jnp.where(left, zb[p, 0, 0, rows, :], zb[p, 1, 0, rows, :])
            high = jnp.where(left, zb[p, 0, 2, rows, :], zb[p, 1, 2, rows, :])
            edge = jnp.where((lane % 64) >= 32, low, high)
            for h in {0: (1,), 1: (0, 1), 2: (0, 1), 3: (0,)}[e]:
                tiles.append(
                    jnp.where(
                        (lane >= 32) & (lane < 96),
                        roll(face, 32 - 64 * h),
                        roll(edge, 96 - 64 * h),
                    )
                )
        return tiles

    def x_pass(p, dst, passes):
        for j in range(TY + 2):
            rows = pl.ds(8 * j, 8)
            col = [f[p, i, rows, :] for i in range(2 * R + BX)]
            for i in range(BX):
                for n, q in enumerate(passes):
                    dst[n, i, rows, :] = q(k, lambda d: col[i + R + d])

    def x_pass_packed(p, dst, passes):
        for j, z in enumerate(packed_in(p)):
            moved = {d: roll(z, -8 * d) for d in range(-R, R + 1)}
            for n, q in enumerate(passes):
                dst[n, pl.ds(8 * j, 8), :] = q(k, lambda d: moved[d])

    def y_at(ref, j):
        return lambda d: ref[pl.ds(8 + 8 * j + d, 8), :]

    def pack_init():
        return {}

    def pack(acc, v, i, j):
        e, h = divmod(j, 2)
        at = 64 * h + 8 * i
        moved = roll(v, at + 4)
        acc[e] = moved if e not in acc else jnp.where((lane >= at) & (lane < at + 8), moved, acc[e])

    def apply(p, use):
        x_pass(p, t, [symmetric])
        x_pass_packed(p, tz, [symmetric])
        for j in range(TY):
            halos = symmetric(k, y_at(tz.at[0], j))
            for i in range(BX):
                own = symmetric(k, y_at(t.at[0, i], j))
                halo = roll(halos, -(8 * (i + R) + 4))
                use(i, j, along_z(own, halo, k, [symmetric])[0])

    def put(p, i, j, v, acc):
        f[p, R + i, pl.ds(8 + 8 * j, 8), :] = v
        pack(acc, v, i, j)

    def flush(p, acc):
        for e, v in acc.items():
            zp[p, pl.ds(8 * e, 8), :] = v

    def ones_sum(index, n):
        acc = None
        for d in range(-R, R + 1):
            ok = (index + d >= 0) & (index + d < n)
            term = jnp.where(ok, k[abs(d)], 0.0)
            acc = term if acc is None else acc + term
        return acc

    sum_z = ones_sum(lane + mz * BZ, nz * BZ)
    sum_y = [ones_sum(sub + (my * BY + 8 * j), ny * BY) * sum_z for j in range(TY)]
    sum_x = [ones_sum(mx * BX + i, nx * BX) for i in range(BX)]

    for c in loads:
        c.wait()
    acc = pack_init()
    total_a, total_b = zero, zero
    for j in range(TY):
        rows = pl.ds(8 * j, 8)
        for i in range(BX):
            a = a_ref[i, rows, :]
            total_a = total_a + a
            total_b = total_b + b_ref[i, rows, :]
            f[1, R + i, pl.ds(8 + 8 * j, 8), :] = jnp.ones((8, BZ), F32)
            put(0, i, j, a / (sum_x[i] * sum_y[j]), acc)
    flush(0, acc)
    tots[0, 0, pl.ds(0, 8), :] = total_a
    tots[0, 0, pl.ds(8, 8), :] = total_b
    pl.semaphore_wait(barrier, expected)
    start(0)
    line("gx", 0, True)

    def v_step(n):
        arrived(0, DIRS)
        acc = pack_init()

        def use(i, j, ku):
            v = f[1, R + i, pl.ds(8 + 8 * j, 8), :]
            w[n, i, pl.ds(8 * j, 8), :] = v * ku
            put(1, i, j, b_ref[i, pl.ds(8 * j, 8), :] / ku, acc)

        apply(0, use)
        flush(1, acc)
        start(1)
        sent(0)

    def u_step():
        arrived(1, DIRS)
        acc = pack_init()

        def use(i, j, kv):
            put(0, i, j, a_ref[i, pl.ds(8 * j, 8), :] / kv, acc)

        apply(1, use)
        flush(0, acc)
        start(0)
        sent(1)

    def iteration(n, carry):
        v_step(n)

        @pl.when(n == 1)
        def _():
            line_end("gx", 0)
            line("gy", 0, True)

        @pl.when(n == 3)
        def _():
            line_end("gy", 0)
            line("gz", 0, True)

        u_step()
        return carry

    lax.fori_loop(0, ITERS - 1, iteration, 0)
    v_step(ITERS - 1)

    line_end("gz", 0)

    def everything(v):
        return jnp.full((8, BZ), cells, F32) / jnp.full((8, BZ), jnp.sum(v), F32)

    alpha = everything(tots[0, 3, pl.ds(0, 8), :])
    beta = everything(tots[0, 3, pl.ds(8, 8), :])
    rows = zero
    for n in range(ITERS):
        part = zero
        for i in range(BX):
            for j in range(TY):
                at = pl.ds(8 * j, 8)
                part = part + jnp.abs(alpha * w[n, i, at, :] - beta * b_ref[i, at, :])
        part = jnp.broadcast_to(jnp.sum(part, axis=0, keepdims=True), (8, BZ))
        rows = jnp.where(sub == n, part, rows)
    tots[1, 0, pl.ds(0, 8), :] = rows
    tots[1, 0, pl.ds(8, 8), :] = zero
    line("gx", 1, True)

    arrived(1, DIRS)
    x_pass(1, t, [symmetric, slope])
    x_pass_packed(1, tz, [symmetric, slope])
    for j in range(TY):
        at = pl.ds(8 + 8 * j, 8)
        halos = [
            symmetric(k, y_at(tz.at[0], j)),
            slope(k, y_at(tz.at[0], j)),
            symmetric(k, y_at(tz.at[1], j)),
        ]
        for i in range(BX):
            by = -(8 * (i + R) + 4)
            kk, kg = symmetric(k, y_at(t.at[0, i], j)), slope(k, y_at(t.at[0, i], j))
            gk = symmetric(k, y_at(t.at[1, i], j))
            kvol, znum = along_z(kk, roll(halos[0], by), k, [symmetric, slope])
            ynum = along_z(kg, roll(halos[1], by), k, [symmetric])[0]
            xnum = along_z(gk, roll(halos[2], by), k, [symmetric])[0]
            inverse = 1.0 / kvol
            for c, num in enumerate((xnum, ynum, znum)):
                xb[c, BX + i, pl.ds(8 * j, 8), :] = num * inverse

    def x_copy(c, d):
        lands = 0 if d > 0 else 2 * BX
        e = 0 if d > 0 else 1
        return pltpu.make_async_remote_copy(
            src_ref=xb.at[c, pl.ds(BX, BX)], dst_ref=xb.at[c, pl.ds(lands, BX)],
            send_sem=xsend.at[c, e], recv_sem=xrecv.at[c, e],
            device_id={"gx": mx + d}, device_id_type=MESH,
        )

    def y_copy(c, d):
        i = YZ.index(d)
        _, dy, dz = d
        if dz == 0:
            ys = pl.ds(BY, 8) if dy > 0 else pl.ds(8, 8)
            yd = pl.ds(0, 8) if dy > 0 else pl.ds(BY + 8, 8)
            source, target = yb.at[c, :, ys], yb.at[c, :, yd]
        else:
            side = 0 if dz > 0 else 1
            rows = {1: pl.ds(BY - 8, 8), -1: pl.ds(0, 8), 0: pl.ds(0, BY)}[dy]
            lands = {1: pl.ds(0, 8), -1: pl.ds(BY + 8, 8), 0: pl.ds(8, BY)}[dy]
            source, target = pz.at[c, rows], zs.at[c, side, lands]
        return pltpu.make_async_remote_copy(
            src_ref=source, dst_ref=target, send_sem=ysend.at[c, i],
            recv_sem=yrecv.at[c, i], device_id=peer(d), device_id_type=MESH,
        )

    for c in range(3):
        for d in (-1, 1):
            @pl.when(conds[0][d])
            def _():
                x_copy(c, d).start()
    sent(1)
    line_end("gx", 1)
    line("gy", 1, True)

    stores = [pltpu.make_async_copy(out.at[c], disp_hbm.at[c], loc.at[2 + c]) for c in range(3)]

    for c in range(3):
        for d in (-1, 1):
            @pl.when(conds[0][-d])
            def _():
                x_copy(c, d).wait_recv()
        for j in range(TY):
            at = pl.ds(8 * j, 8)
            packed = None
            for i in range(BX):
                v = symmetric(s, lambda d: xb[c, BX + i + d, at, :])
                yb[c, i, pl.ds(8 + 8 * j, 8), :] = v
                moved = roll(v, 16 * i + 8)
                packed = moved if packed is None else jnp.where(
                    (lane >= 16 * i) & (lane < 16 * i + 16), moved, packed
                )
            pz[c, at, :] = packed
        for d in YZ:
            @pl.when(has(d))
            def _():
                y_copy(c, d).start()
        if c == 0:
            line_end("gy", 1)
            line("gz", 1, True)

    for c in range(3):
        for d in YZ:
            @pl.when(has(neg(d)))
            def _():
                y_copy(c, d).wait_recv()
        for j in range(TY + 2):
            at = pl.ds(8 * j, 8)
            tz2[at, :] = jnp.where((lane % 16) < S, zs[c, 0, at, :], zs[c, 1, at, :])
        for j in range(TY):
            halos = symmetric(s, y_at(tz2, j))
            for i in range(BX):
                own = symmetric(s, y_at(yb.at[c, i], j))
                out[c, i, pl.ds(8 * j, 8), :] = along_z(
                    own, roll(halos, -(16 * i + 8)), s, [symmetric]
                )[0]
        stores[c].start()

    line_end("gz", 1)
    done = tots[1, 3, pl.ds(0, 8), :]
    for n in range(ITERS):
        mis[n] = jnp.sum(jnp.where(sub == n, done, 0.0)) / cells
    for c in range(3):
        for d in (-1, 1):
            @pl.when(conds[0][d])
            def _():
                x_copy(c, d).wait_send()
        for d in YZ:
            @pl.when(has(d))
            def _():
                y_copy(c, d).wait_send()
        stores[c].wait()


def solution(mesh):
    sizes = tuple(mesh.shape[a] for a in ("gx", "gy", "gz"))
    peers = sum(sizes) - 3

    def step(source, target, kernel_half, smooth_half):
        return pl.pallas_call(
            functools.partial(kernel, sizes),
            out_shape=(
                jax.ShapeDtypeStruct((3, BX, BY, BZ), F32),
                jax.ShapeDtypeStruct((ITERS,), F32),
            ),
            in_specs=[
                pl.BlockSpec(memory_space=pl.ANY),
                pl.BlockSpec(memory_space=pl.ANY),
                pl.BlockSpec(memory_space=pltpu.SMEM),
                pl.BlockSpec(memory_space=pltpu.SMEM),
            ],
            out_specs=(
                pl.BlockSpec(memory_space=pl.ANY),
                pl.BlockSpec(memory_space=pltpu.SMEM),
            ),
            scratch_shapes=[
                pltpu.VMEM((BX, BY, BZ), F32),
                pltpu.VMEM((BX, BY, BZ), F32),
                pltpu.VMEM((2, BX + 2 * R, BY + 16, BZ), F32),
                pltpu.VMEM((2, 16, BZ), F32),
                pltpu.VMEM((2, 2, 3, 32, BZ), F32),
                pltpu.VMEM((2, BX, BY + 16, BZ), F32),
                pltpu.VMEM((2, BY + 16, BZ), F32),
                pltpu.VMEM((ITERS, BX, BY, BZ), F32),
                pltpu.VMEM((2, 4, 16, BZ), F32),
                pltpu.VMEM((2, peers, 16, BZ), F32),
                pltpu.VMEM((3, BX, BY, BZ), F32),
                pltpu.VMEM((3, 3 * BX, BY, BZ), F32),
                pltpu.VMEM((3, BX, BY + 16, BZ), F32),
                pltpu.VMEM((3, BY, BZ), F32),
                pltpu.VMEM((3, 2, BY + 16, BZ), F32),
                pltpu.VMEM((8, BZ), F32),
                pltpu.VMEM((BY + 16, BZ), F32),
                pltpu.SemaphoreType.DMA((2, 26)),
                pltpu.SemaphoreType.DMA((2, 26)),
                pltpu.SemaphoreType.DMA((3, 2)),
                pltpu.SemaphoreType.DMA((3, 2)),
                pltpu.SemaphoreType.DMA((3, 8)),
                pltpu.SemaphoreType.DMA((3, 8)),
                pltpu.SemaphoreType.DMA((2, peers)),
                pltpu.SemaphoreType.DMA((2, peers)),
                pltpu.SemaphoreType.DMA((5,)),
            ],
            compiler_params=pltpu.CompilerParams(
                collective_id=0, has_side_effects=True, vmem_limit_bytes=32 * 1024 * 1024
            ),
        )(source, target, kernel_half, smooth_half)

    placed = P("gx", "gy", "gz")
    return jax.shard_map(
        step,
        mesh=mesh,
        in_specs=(placed, placed, P(), P()),
        out_specs=(P(None, "gx", "gy", "gz"), P()),
        check_vma=False,
    )
```

```python
import functools

import jax
import jax.numpy as jnp
from jax import lax
from jax.experimental import pallas as pl
from jax.experimental.pallas import tpu as pltpu
from jax.sharding import PartitionSpec as P

ITERS = 6
R = 4
S = 8
BX, BY, BZ = 8, 32, 128
TY = BY // 8
MESH = pl.DeviceIdType.MESH
F32 = jnp.float32

DIRS = sorted(
    [
        (dx, dy, dz)
        for dx in (-1, 0, 1)
        for dy in (-1, 0, 1)
        for dz in (-1, 0, 1)
        if (dx, dy, dz) != (0, 0, 0)
    ],
    key=lambda d: (-sum(abs(c) for c in d), abs(d[0]), abs(d[1]), d),
)
YZ = [d for d in DIRS if d[0] == 0]


def kernel(
    sizes,
    src_hbm, tgt_hbm, kern_hbm, smo_hbm,
    out, mis,
    a_ref, b_ref, kern, smo, f, zp, zb, t, tz, w, tots, totb, inv,
    xb, yb, pz, zs, tz2,
    send, recv, xsend, xrecv, ysend, yrecv, lsend, lrecv, loc,
):
    nx, ny, nz = sizes
    cells = float(nx * ny * nz * BX * BY * BZ)
    mx, my, mz = lax.axis_index("gx"), lax.axis_index("gy"), lax.axis_index("gz")
    pos = {"gx": (mx, nx), "gy": (my, ny), "gz": (mz, nz)}
    lane = lax.broadcasted_iota(jnp.int32, (8, BZ), 1)
    sub = lax.broadcasted_iota(jnp.int32, (8, BZ), 0)
    zero = jnp.zeros((8, BZ), F32)

    loads = [
        pltpu.make_async_copy(src_hbm, a_ref, loc.at[0]),
        pltpu.make_async_copy(tgt_hbm, b_ref, loc.at[1]),
        pltpu.make_async_copy(kern_hbm, kern, loc.at[2]),
        pltpu.make_async_copy(smo_hbm, smo, loc.at[3]),
    ]
    for c in loads:
        c.start()

    def inside(m, n, d):
        if d == 0:
            return None
        return m + d < n if d > 0 else m + d >= 0

    conds = [{d: inside(m, n, d) for d in (-1, 0, 1)} for m, n in pos.values()]

    def has(d):
        c = [conds[i][d[i]] for i in range(3) if d[i]]
        return functools.reduce(jnp.logical_and, c)

    def peer(d):
        ids = {}
        for axis, step in zip(pos, d):
            if step:
                ids[axis] = pos[axis][0] + step
        return ids

    def neg(d):
        return tuple(-c for c in d)

    for p in range(2):
        for i in range(2 * R + BX):
            for j in range(TY + 2):
                f[p, i, pl.ds(8 * j, 8), :] = zero
        for q in range(2):
            for e in range(3):
                for j in range(4):
                    zb[p, q, e, pl.ds(8 * j, 8), :] = zero

    barrier = pltpu.get_barrier_semaphore()
    expected = 0
    for d in DIRS:
        there = has(d)
        expected = expected + jnp.where(there, 1, 0)

        @pl.when(there)
        def _():
            pl.semaphore_signal(barrier, 1, device_id=peer(d), device_id_type=MESH)

    for c in range(3):
        for i in range(BX):
            for j in range(TY):
                xb[c, i, pl.ds(8 * j, 8), :] = zero
                xb[c, 2 * BX + i, pl.ds(8 * j, 8), :] = zero
            for j in (0, TY + 1):
                yb[c, i, pl.ds(8 * j, 8), :] = zero
        for q in range(2):
            for j in range(TY + 2):
                zs[c, q, pl.ds(8 * j, 8), :] = zero

    for c in loads[2:]:
        c.wait()
    k = [kern[i] for i in range(R + 1)]
    norm = smo[0]
    tail = smo[1]
    for i in range(2, S + 1):
        tail = tail + smo[i]
    norm = jnp.full((8, BZ), norm + 2.0 * tail, F32)
    s = [jnp.full((8, BZ), smo[i], F32) / norm for i in range(S + 1)]

    def copy(p, d):
        i = DIRS.index(d)
        dx, dy, dz = d
        if dz == 0:
            xs = {1: pl.ds(BX, R), -1: pl.ds(R, R), 0: pl.ds(R, BX)}[dx]
            xd = {1: pl.ds(0, R), -1: pl.ds(R + BX, R), 0: pl.ds(R, BX)}[dx]
            ys = {1: pl.ds(BY + 8 - R, R), -1: pl.ds(8, R), 0: pl.ds(8, BY)}[dy]
            yd = {1: pl.ds(8 - R, R), -1: pl.ds(BY + 8, R), 0: pl.ds(8, BY)}[dy]
            source, target = f.at[p, xs, ys], f.at[p, xd, yd]
        else:
            side = 0 if dz > 0 else 1
            rows = {1: pl.ds(8, 8), -1: pl.ds(0, 8), 0: pl.ds(0, 16)}[dx]
            lands = {1: pl.ds(0, 8), -1: pl.ds(24, 8), 0: pl.ds(8, 16)}[dx]
            source, target = zp.at[p, rows], zb.at[p, side, 1 - dy, lands]
        return pltpu.make_async_remote_copy(
            src_ref=source, dst_ref=target, send_sem=send.at[p, i],
            recv_sem=recv.at[p, i], device_id=peer(d), device_id_type=MESH,
        )

    def start(p):
        for d in DIRS:
            @pl.when(has(d))
            def _():
                copy(p, d).start()

    def sent(p):
        for d in DIRS:
            @pl.when(has(d))
            def _():
                copy(p, d).wait_send()

    def arrived(p, dirs):
        for d in dirs:
            @pl.when(has(neg(d)))
            def _():
                copy(p, d).wait_recv()

    def line(axis, q, go):
        m, n = pos[axis]
        base = {"gx": 0, "gy": nx - 1, "gz": nx + ny - 2}[axis]
        for j in range(1, n):
            c = pltpu.make_async_remote_copy(
                src_ref=tots.at[q, "xyz".index(axis[1])], dst_ref=totb.at[q, base + j - 1],
                send_sem=lsend.at[q, base + j - 1], recv_sem=lrecv.at[q, base + j - 1],
                device_id={axis: lax.rem(m + j, n)}, device_id_type=MESH,
            )
            if go:
                c.start()
            else:
                c.wait()

    def line_end(axis, q):
        line(axis, q, False)
        n = pos[axis][1]
        a = "xyz".index(axis[1])
        base = {"gx": 0, "gy": nx - 1, "gz": nx + ny - 2}[axis]
        v = tots[q, a]
        for j in range(1, n):
            v = v + totb[q, base + j - 1]
        tots[q, a + 1] = v

    def symmetric(taps, at):
        acc = taps[0] * at(0)
        for d in range(1, len(taps)):
            acc = acc + taps[d] * (at(d) + at(-d))
        return acc

    def slope(taps, at):
        acc = None
        for d in range(1, len(taps)):
            term = (float(d) * taps[d]) * (at(d) - at(-d))
            acc = term if acc is None else acc + term
        return acc

    def roll(v, by):
        by = by % BZ
        return v if by == 0 else pltpu.roll(v, by, 1)

    def along_z(own, halo, taps, passes):
        n = len(taps)
        shifted = {0: own}
        for d in range(1, n):
            shifted[d] = roll(jnp.where(lane < d, halo, own), -d)
            shifted[-d] = roll(jnp.where(lane >= BZ - d, halo, own), d)
        return [q(taps, lambda d: shifted[d]) for q in passes]

    def packed_in(p):
        left = (lane % 8) < R
        tiles = []
        for e, hs in enumerate(((TY - 1,), range(TY), (0,))):
            parts = [
                jnp.where(left, zb[p, 0, e, pl.ds(8 * g, 8), :], zb[p, 1, e, pl.ds(8 * g, 8), :])
                for g in range(4)
            ]
            for h in hs:
                moved = [roll(parts[g], 32 * (g - h)) for g in range(4)]
                tiles.append(
                    jnp.where(
                        lane < 64,
                        jnp.where(lane < 32, moved[0], moved[1]),
                        jnp.where(lane < 96, moved[2], moved[3]),
                    )
                )
        return tiles

    def x_pass(p, dst, passes):
        for j in range(TY + 2):
            rows = pl.ds(8 * j, 8)
            col = [f[p, i, rows, :] for i in range(2 * R + BX)]
            for i in range(BX):
                for n, q in enumerate(passes):
                    dst[n, i, rows, :] = q(k, lambda d: col[i + R + d])

    def x_pass_packed(p, dst, passes):
        for j, z in enumerate(packed_in(p)):
            moved = {d: roll(z, -8 * d) for d in range(-R, R + 1)}
            for n, q in enumerate(passes):
                dst[n, pl.ds(8 * j, 8), :] = q(k, lambda d: moved[d])

    def y_at(ref, j):
        return lambda d: ref[pl.ds(8 + 8 * j + d, 8), :]

    def pack_init():
        return {}

    def pack(acc, v, i, j):
        e, g = divmod(i, 4)
        at = 32 * j + 8 * g
        moved = roll(v, at + 4)
        acc[e] = moved if e not in acc else jnp.where((lane >= at) & (lane < at + 8), moved, acc[e])

    def apply(p, use):
        x_pass(p, t, [symmetric])
        x_pass_packed(p, tz, [symmetric])
        for j in range(TY):
            halos = symmetric(k, y_at(tz.at[0], j))
            for i in range(BX):
                own = symmetric(k, y_at(t.at[0, i], j))
                halo = roll(halos, -(8 * (i + R) + 4))
                use(i, j, along_z(own, halo, k, [symmetric])[0])

    def put(p, i, j, v, acc):
        f[p, R + i, pl.ds(8 + 8 * j, 8), :] = v
        pack(acc, v, i, j)

    def flush(p, acc):
        for e, v in acc.items():
            zp[p, pl.ds(8 * e, 8), :] = v

    def ones_sum(index, n):
        acc = None
        for d in range(-R, R + 1):
            ok = (index + d >= 0) & (index + d < n)
            term = jnp.where(ok, k[abs(d)], 0.0)
            acc = term if acc is None else acc + term
        return acc

    sum_z = ones_sum(lane + mz * BZ, nz * BZ)
    sum_y = [ones_sum(sub + (my * BY + 8 * j), ny * BY) * sum_z for j in range(TY)]
    sum_x = [ones_sum(mx * BX + i, nx * BX) for i in range(BX)]

    for c in loads[:2]:
        c.wait()
    acc = pack_init()
    total_a, total_b = zero, zero
    for j in range(TY):
        rows = pl.ds(8 * j, 8)
        for i in range(BX):
            a = a_ref[i, rows, :]
            total_a = total_a + a
            total_b = total_b + b_ref[i, rows, :]
            f[1, R + i, pl.ds(8 + 8 * j, 8), :] = jnp.ones((8, BZ), F32)
            put(0, i, j, a / (sum_x[i] * sum_y[j]), acc)
    flush(0, acc)
    total_a = jnp.broadcast_to(jnp.sum(total_a, axis=0, keepdims=True), (8, BZ))
    total_b = jnp.broadcast_to(jnp.sum(total_b, axis=0, keepdims=True), (8, BZ))
    tots[0, 0] = jnp.where(sub == 0, total_a, jnp.where(sub == 1, total_b, zero))
    pl.semaphore_wait(barrier, expected)
    start(0)

    def v_step(n):
        arrived(0, DIRS)
        acc = pack_init()

        def use(i, j, ku):
            v = f[1, R + i, pl.ds(8 + 8 * j, 8), :]
            w[n, i, pl.ds(8 * j, 8), :] = v * ku
            put(1, i, j, b_ref[i, pl.ds(8 * j, 8), :] / ku, acc)

        apply(0, use)
        flush(1, acc)
        start(1)
        sent(0)

    def u_step():
        arrived(1, DIRS)
        acc = pack_init()

        def use(i, j, kv):
            put(0, i, j, a_ref[i, pl.ds(8 * j, 8), :] / kv, acc)

        apply(1, use)
        flush(0, acc)
        start(0)
        sent(1)

    def iteration(n, carry):
        v_step(n)

        @pl.when(n == 3)
        def _():
            line("gx", 0, True)

        @pl.when(n == 4)
        def _():
            line_end("gy", 0)
            line("gz", 0, True)

        u_step()

        @pl.when(n == 3)
        def _():
            line_end("gx", 0)
            line("gy", 0, True)

        return carry

    lax.fori_loop(0, ITERS - 1, iteration, 0)
    v_step(ITERS - 1)

    line_end("gz", 0)

    def everything(row):
        v = jnp.where(sub == row, tots[0, 3], zero)
        return jnp.full((8, BZ), cells, F32) / jnp.full((8, BZ), jnp.sum(v), F32)

    alpha, beta = everything(0), everything(1)
    rows = zero
    for n in range(ITERS):
        part = zero
        for i in range(BX):
            for j in range(TY):
                at = pl.ds(8 * j, 8)
                part = part + jnp.abs(alpha * w[n, i, at, :] - beta * b_ref[i, at, :])
        part = jnp.broadcast_to(jnp.sum(part, axis=0, keepdims=True), (8, BZ))
        rows = jnp.where(sub == n, part, rows)
    tots[1, 0] = rows
    line("gx", 1, True)

    def x_copy(c, d):
        lands = 0 if d > 0 else 2 * BX
        e = 0 if d > 0 else 1
        return pltpu.make_async_remote_copy(
            src_ref=xb.at[c, pl.ds(BX, BX)], dst_ref=xb.at[c, pl.ds(lands, BX)],
            send_sem=xsend.at[c, e], recv_sem=xrecv.at[c, e],
            device_id={"gx": mx + d}, device_id_type=MESH,
        )

    def y_copy(c, d):
        i = YZ.index(d)
        _, dy, dz = d
        if dz == 0:
            ys = pl.ds(BY, 8) if dy > 0 else pl.ds(8, 8)
            yd = pl.ds(0, 8) if dy > 0 else pl.ds(BY + 8, 8)
            source, target = yb.at[c, :, ys], yb.at[c, :, yd]
        else:
            side = 0 if dz > 0 else 1
            rows = {1: pl.ds(BY - 8, 8), -1: pl.ds(0, 8), 0: pl.ds(0, BY)}[dy]
            lands = {1: pl.ds(0, 8), -1: pl.ds(BY + 8, 8), 0: pl.ds(8, BY)}[dy]
            source, target = pz.at[c, rows], zs.at[c, side, lands]
        return pltpu.make_async_remote_copy(
            src_ref=source, dst_ref=target, send_sem=ysend.at[c, i],
            recv_sem=yrecv.at[c, i], device_id=peer(d), device_id_type=MESH,
        )

    def x_start(c):
        for d in (-1, 1):
            @pl.when(conds[0][d])
            def _():
                x_copy(c, d).start()

    def x_arrived(c):
        for d in (-1, 1):
            @pl.when(conds[0][-d])
            def _():
                x_copy(c, d).wait_recv()

    def y_start(c):
        for d in YZ:
            @pl.when(has(d))
            def _():
                y_copy(c, d).start()

    def y_arrived(c):
        for d in YZ:
            @pl.when(has(neg(d)))
            def _():
                y_copy(c, d).wait_recv()

    def y_put(c, value):
        for j in range(TY):
            packed = None
            for i in range(BX):
                v = value(i, j)
                yb[c, i, pl.ds(8 + 8 * j, 8), :] = v
                moved = roll(v, 16 * i + 8)
                packed = moved if packed is None else jnp.where(
                    (lane >= 16 * i) & (lane < 16 * i + 16), moved, packed
                )
            pz[c, pl.ds(8 * j, 8), :] = packed

    def smooth_x(c, i, j):
        return symmetric(s, lambda d: xb[c, BX + i + d, pl.ds(8 * j, 8), :])

    def smooth_yz(c, put_value):
        for j in range(TY + 2):
            at = pl.ds(8 * j, 8)
            tz2[at, :] = jnp.where((lane % 16) < S, zs[c, 0, at, :], zs[c, 1, at, :])
        for j in range(TY):
            halos = symmetric(s, y_at(tz2, j))
            for i in range(BX):
                own = symmetric(s, y_at(yb.at[c, i], j))
                put_value(i, j, along_z(own, roll(halos, -(16 * i + 8)), s, [symmetric])[0])

    def at_z(i, halos):
        return roll(halos, -(8 * (i + R) + 4))

    arrived(1, DIRS)
    x_pass(1, t, [symmetric, slope])
    x_pass_packed(1, tz, [symmetric, slope])
    for j in range(TY):
        halos = symmetric(k, y_at(tz.at[0], j))
        for i in range(BX):
            kk = symmetric(k, y_at(t.at[0, i], j))
            kvol, znum = along_z(kk, at_z(i, halos), k, [symmetric, slope])
            inverse = 1.0 / kvol
            inv[i, pl.ds(8 * j, 8), :] = inverse
            xb[2, BX + i, pl.ds(8 * j, 8), :] = znum * inverse
    x_start(2)

    halos = [slope(k, y_at(tz.at[0], j)) for j in range(TY)]

    def raw_y(i, j):
        kg = slope(k, y_at(t.at[0, i], j))
        return along_z(kg, at_z(i, halos[j]), k, [symmetric])[0] * inv[i, pl.ds(8 * j, 8), :]

    y_put(1, raw_y)
    y_start(1)

    for j in range(TY):
        halos = symmetric(k, y_at(tz.at[1], j))
        for i in range(BX):
            gk = symmetric(k, y_at(t.at[1, i], j))
            xnum = along_z(gk, at_z(i, halos), k, [symmetric])[0]
            xb[0, BX + i, pl.ds(8 * j, 8), :] = xnum * inv[i, pl.ds(8 * j, 8), :]
    x_start(0)
    sent(1)
    line_end("gx", 1)
    line("gy", 1, True)

    y_arrived(1)

    def to_x(i, j, v):
        xb[1, BX + i, pl.ds(8 * j, 8), :] = v

    smooth_yz(1, to_x)
    x_start(1)
    line_end("gy", 1)
    line("gz", 1, True)

    def to_out(c):
        def put_value(i, j, v):
            out[c, i, pl.ds(8 * j, 8), :] = v

        return put_value

    for c in (2, 0):
        x_arrived(c)
        y_put(c, functools.partial(smooth_x, c))
        y_start(c)
    y_arrived(2)
    smooth_yz(2, to_out(2))
    x_arrived(1)
    for j in range(TY):
        for i in range(BX):
            to_out(1)(i, j, smooth_x(1, i, j))
    y_arrived(0)
    smooth_yz(0, to_out(0))

    line_end("gz", 1)
    done = tots[1, 3]
    for n in range(ITERS):
        mis[n] = jnp.sum(jnp.where(sub == n, done, 0.0)) / cells
    for c in range(3):
        for d in (-1, 1):
            @pl.when(conds[0][d])
            def _():
                x_copy(c, d).wait_send()
        for d in YZ:
            @pl.when(has(d))
            def _():
                y_copy(c, d).wait_send()


def solution(mesh):
    sizes = tuple(mesh.shape[a] for a in ("gx", "gy", "gz"))
    peers = sum(sizes) - 3

    def step(source, target, kernel_half, smooth_half):
        return pl.pallas_call(
            functools.partial(kernel, sizes),
            out_shape=(
                jax.ShapeDtypeStruct((3, BX, BY, BZ), F32),
                jax.ShapeDtypeStruct((ITERS,), F32),
            ),
            in_specs=[pl.BlockSpec(memory_space=pltpu.HBM)] * 4,
            out_specs=(
                pl.BlockSpec(memory_space=pltpu.VMEM),
                pl.BlockSpec(memory_space=pltpu.SMEM),
            ),
            scratch_shapes=[
                pltpu.VMEM((BX, BY, BZ), F32),
                pltpu.VMEM((BX, BY, BZ), F32),
                pltpu.SMEM((R + 1,), F32),
                pltpu.SMEM((S + 1,), F32),
                pltpu.VMEM((2, BX + 2 * R, BY + 16, BZ), F32),
                pltpu.VMEM((2, 16, BZ), F32),
                pltpu.VMEM((2, 2, 3, 32, BZ), F32),
                pltpu.VMEM((2, BX, BY + 16, BZ), F32),
                pltpu.VMEM((2, BY + 16, BZ), F32),
                pltpu.VMEM((ITERS, BX, BY, BZ), F32),
                pltpu.VMEM((2, 4, 8, BZ), F32),
                pltpu.VMEM((2, peers, 8, BZ), F32),
                pltpu.VMEM((BX, BY, BZ), F32),
                pltpu.VMEM((3, 3 * BX, BY, BZ), F32),
                pltpu.VMEM((3, BX, BY + 16, BZ), F32),
                pltpu.VMEM((3, BY, BZ), F32),
                pltpu.VMEM((3, 2, BY + 16, BZ), F32),
                pltpu.VMEM((BY + 16, BZ), F32),
                pltpu.SemaphoreType.DMA((2, 26)),
                pltpu.SemaphoreType.DMA((2, 26)),
                pltpu.SemaphoreType.DMA((3, 2)),
                pltpu.SemaphoreType.DMA((3, 2)),
                pltpu.SemaphoreType.DMA((3, 8)),
                pltpu.SemaphoreType.DMA((3, 8)),
                pltpu.SemaphoreType.DMA((2, peers)),
                pltpu.SemaphoreType.DMA((2, peers)),
                pltpu.SemaphoreType.DMA((4,)),
            ],
            compiler_params=pltpu.CompilerParams(
                collective_id=0, has_side_effects=True, vmem_limit_bytes=67043328
            ),
        )(source, target, kernel_half, smooth_half)

    placed = P("gx", "gy", "gz")
    return jax.shard_map(
        step,
        mesh=mesh,
        in_specs=(placed, placed, P(), P()),
        out_specs=(P(None, "gx", "gy", "gz"), P()),
        check_vma=False,
    )
```

```python
import functools

import jax
import jax.numpy as jnp
from jax import lax
from jax.experimental import pallas as pl
from jax.experimental.pallas import tpu as pltpu
from jax.sharding import PartitionSpec as P

ITERS = 6
R = 4
S = 8
BX, BY, BZ = 8, 32, 128
TY = BY // 8
MESH = pl.DeviceIdType.MESH
F32 = jnp.float32

DIRS = sorted(
    [
        (dx, dy, dz)
        for dx in (-1, 0, 1)
        for dy in (-1, 0, 1)
        for dz in (-1, 0, 1)
        if (dx, dy, dz) != (0, 0, 0)
    ],
    key=lambda d: (-sum(abs(c) for c in d), abs(d[0]), abs(d[1]), d),
)
YZ = [d for d in DIRS if d[0] == 0]
SMALL = [d for d in DIRS if d[1:] != (0, 0)]


def kernel(
    sizes,
    src_hbm, tgt_hbm, kern_hbm, smo_hbm,
    out, mis,
    a_ref, b_ref, kern, smo, f, zp, zb, t, tz, w, tots, totb, inv,
    xb, yb, pz, zs, tz2,
    send, recv, fsend, frecv, xsend, xrecv, ysend, yrecv, lsend, lrecv, loc,
):
    nx, ny, nz = sizes
    cells = float(nx * ny * nz * BX * BY * BZ)
    mx, my, mz = lax.axis_index("gx"), lax.axis_index("gy"), lax.axis_index("gz")
    pos = {"gx": (mx, nx), "gy": (my, ny), "gz": (mz, nz)}
    lane = lax.broadcasted_iota(jnp.int32, (8, BZ), 1)
    sub = lax.broadcasted_iota(jnp.int32, (8, BZ), 0)
    zero = jnp.zeros((8, BZ), F32)

    loads = [
        pltpu.make_async_copy(src_hbm, a_ref, loc.at[0]),
        pltpu.make_async_copy(tgt_hbm, b_ref, loc.at[1]),
        pltpu.make_async_copy(kern_hbm, kern, loc.at[2]),
        pltpu.make_async_copy(smo_hbm, smo, loc.at[3]),
    ]
    for c in loads:
        c.start()

    def inside(m, n, d):
        if d == 0:
            return None
        return m + d < n if d > 0 else m + d >= 0

    conds = [{d: inside(m, n, d) for d in (-1, 0, 1)} for m, n in pos.values()]

    def has(d):
        c = [conds[i][d[i]] for i in range(3) if d[i]]
        return functools.reduce(jnp.logical_and, c)

    def peer(d):
        ids = {}
        for axis, step in zip(pos, d):
            if step:
                ids[axis] = pos[axis][0] + step
        return ids

    def neg(d):
        return tuple(-c for c in d)

    for p in range(2):
        for i in range(3 * R + BX):
            for j in range(TY + 2):
                f[p, i, pl.ds(8 * j, 8), :] = zero
        for q in range(2):
            for e in range(3):
                for j in range(4):
                    zb[p, q, e, pl.ds(8 * j, 8), :] = zero

    barrier = pltpu.get_barrier_semaphore()
    expected = 0
    for d in DIRS:
        there = has(d)
        expected = expected + jnp.where(there, 1, 0)

        @pl.when(there)
        def _():
            pl.semaphore_signal(barrier, 1, device_id=peer(d), device_id_type=MESH)

    for c in range(3):
        for i in range(BX):
            for j in range(TY):
                xb[c, i, pl.ds(8 * j, 8), :] = zero
                xb[c, 2 * BX + i, pl.ds(8 * j, 8), :] = zero
            for j in (0, TY + 1):
                yb[c, i, pl.ds(8 * j, 8), :] = zero
        for q in range(2):
            for j in range(TY + 2):
                zs[c, q, pl.ds(8 * j, 8), :] = zero

    for c in loads[2:]:
        c.wait()
    k = [kern[i] for i in range(R + 1)]
    norm = smo[0]
    tail = smo[1]
    for i in range(2, S + 1):
        tail = tail + smo[i]
    norm = jnp.full((8, BZ), norm + 2.0 * tail, F32)
    s = [jnp.full((8, BZ), smo[i], F32) / norm for i in range(S + 1)]

    def copy(p, d):
        i = DIRS.index(d)
        dx, dy, dz = d
        if dz == 0:
            xs = {1: pl.ds(BX, R), -1: pl.ds(R, R), 0: pl.ds(R, BX)}[dx]
            xd = {1: pl.ds(0, R), -1: pl.ds(R + BX, R), 0: pl.ds(R, BX)}[dx]
            ys = {1: pl.ds(BY + 8 - R, R), -1: pl.ds(8, R), 0: pl.ds(8, BY)}[dy]
            yd = {1: pl.ds(8 - R, R), -1: pl.ds(BY + 8, R), 0: pl.ds(8, BY)}[dy]
            source, target = f.at[p, xs, ys], f.at[p, xd, yd]
        else:
            side = 0 if dz > 0 else 1
            rows = {1: pl.ds(8, 8), -1: pl.ds(0, 8), 0: pl.ds(0, 16)}[dx]
            lands = {1: pl.ds(0, 8), -1: pl.ds(24, 8), 0: pl.ds(8, 16)}[dx]
            source, target = zp.at[p, rows], zb.at[p, side, 1 - dy, lands]
        return pltpu.make_async_remote_copy(
            src_ref=source, dst_ref=target, send_sem=send.at[p, i],
            recv_sem=recv.at[p, i], device_id=peer(d), device_id_type=MESH,
        )

    other = mz + 1 - 2 * lax.rem(mz, 2)

    def face(p, d, j):
        ok = conds[0][d]
        near, far = (R + BX, 0) if d < 0 else (0, R + BX)
        e = jnp.where(ok, near, far)
        source = jnp.where(ok, BX if d > 0 else R, 2 * R + BX)
        side = jnp.where(ok, 0 if d > 0 else 1, 1 if d > 0 else 0)
        rows = pl.ds(8 + 8 * j, 8)
        return pltpu.make_async_remote_copy(
            src_ref=f.at[p, pl.ds(source, R), rows], dst_ref=f.at[p, pl.ds(e, R), rows],
            send_sem=fsend.at[p, 0 if d > 0 else 1, j], recv_sem=frecv.at[p, side, j],
            device_id={"gx": jnp.where(ok, mx + d, mx), "gz": jnp.where(ok, mz, other)},
            device_id_type=MESH,
        )

    def face_start(p, j):
        for d in (1, -1):
            face(p, d, j).start()

    def face_arrived(p, j):
        rows = pl.ds(8 + 8 * j, 8)
        for side, at in ((0, 0), (1, R + BX)):
            pltpu.make_async_remote_copy(
                src_ref=f.at[p, pl.ds(BX, R), rows], dst_ref=f.at[p, pl.ds(at, R), rows],
                send_sem=fsend.at[p, side, j], recv_sem=frecv.at[p, side, j],
                device_id={"gz": other}, device_id_type=MESH,
            ).wait_recv()

    def start(p):
        for d in SMALL:
            @pl.when(has(d))
            def _():
                copy(p, d).start()

    def sent(p):
        for d in SMALL:
            @pl.when(has(d))
            def _():
                copy(p, d).wait_send()
        for j in range(TY):
            for d in (1, -1):
                face(p, d, j).wait_send()

    def arrived(p, dirs):
        for d in dirs:
            @pl.when(has(neg(d)))
            def _():
                copy(p, d).wait_recv()

    def line(axis, q, go):
        m, n = pos[axis]
        base = {"gx": 0, "gy": nx - 1, "gz": nx + ny - 2}[axis]
        for j in range(1, n):
            c = pltpu.make_async_remote_copy(
                src_ref=tots.at[q, "xyz".index(axis[1])], dst_ref=totb.at[q, base + j - 1],
                send_sem=lsend.at[q, base + j - 1], recv_sem=lrecv.at[q, base + j - 1],
                device_id={axis: lax.rem(m + j, n)}, device_id_type=MESH,
            )
            if go:
                c.start()
            else:
                c.wait()

    def line_end(axis, q):
        line(axis, q, False)
        n = pos[axis][1]
        a = "xyz".index(axis[1])
        base = {"gx": 0, "gy": nx - 1, "gz": nx + ny - 2}[axis]
        v = tots[q, a]
        for j in range(1, n):
            v = v + totb[q, base + j - 1]
        tots[q, a + 1] = v

    def symmetric(taps, at):
        acc = taps[0] * at(0)
        for d in range(1, len(taps)):
            acc = acc + taps[d] * (at(d) + at(-d))
        return acc

    def slope(taps, at):
        acc = None
        for d in range(1, len(taps)):
            term = (float(d) * taps[d]) * (at(d) - at(-d))
            acc = term if acc is None else acc + term
        return acc

    def roll(v, by):
        by = by % BZ
        return v if by == 0 else pltpu.roll(v, by, 1)

    def along_z(own, halo, taps, passes):
        n = len(taps)
        shifted = {0: own}
        for d in range(1, n):
            shifted[d] = roll(jnp.where(lane < d, halo, own), -d)
            shifted[-d] = roll(jnp.where(lane >= BZ - d, halo, own), d)
        return [q(taps, lambda d: shifted[d]) for q in passes]

    def packed_in(p):
        left = (lane % 8) < R
        tiles = []
        for e, hs in enumerate(((TY - 1,), range(TY), (0,))):
            parts = [
                jnp.where(left, zb[p, 0, e, pl.ds(8 * g, 8), :], zb[p, 1, e, pl.ds(8 * g, 8), :])
                for g in range(4)
            ]
            for h in hs:
                moved = [roll(parts[g], 32 * (g - h)) for g in range(4)]
                tiles.append(
                    jnp.where(
                        lane < 64,
                        jnp.where(lane < 32, moved[0], moved[1]),
                        jnp.where(lane < 96, moved[2], moved[3]),
                    )
                )
        return tiles

    def x_tile(p, j, dst, passes):
        rows = pl.ds(8 * j, 8)
        col = [f[p, i, rows, :] for i in range(2 * R + BX)]
        for i in range(BX):
            for n, q in enumerate(passes):
                dst[n, i, rows, :] = q(k, lambda d: col[i + R + d])

    def x_pass_packed(p, dst, passes):
        for j, z in enumerate(packed_in(p)):
            moved = {d: roll(z, -8 * d) for d in range(-R, R + 1)}
            for n, q in enumerate(passes):
                dst[n, pl.ds(8 * j, 8), :] = q(k, lambda d: moved[d])

    def y_at(ref, j):
        return lambda d: ref[pl.ds(8 + 8 * j + d, 8), :]

    def pack_init():
        return {}

    def pack(acc, v, i, j):
        e, g = divmod(i, 4)
        at = 32 * j + 8 * g
        moved = roll(v, at + 4)
        acc[e] = moved if e not in acc else jnp.where((lane >= at) & (lane < at + 8), moved, acc[e])

    def apply(p, use, after):
        arrived(p, SMALL)
        for j in (0, TY + 1):
            x_tile(p, j, t, [symmetric])
        x_pass_packed(p, tz, [symmetric])
        halos = [symmetric(k, y_at(tz.at[0], j)) for j in range(TY)]

        def row(j):
            for i in range(BX):
                own = symmetric(k, y_at(t.at[0, i], j))
                halo = roll(halos[j], -(8 * (i + R) + 4))
                use(i, j, along_z(own, halo, k, [symmetric])[0])
            after(j)

        for j in range(TY):
            face_arrived(p, j)
            x_tile(p, j + 1, t, [symmetric])
            if j:
                row(j - 1)
        row(TY - 1)

    def put(p, i, j, v, acc):
        f[p, R + i, pl.ds(8 + 8 * j, 8), :] = v
        pack(acc, v, i, j)

    def flush(p, acc):
        for e, v in acc.items():
            zp[p, pl.ds(8 * e, 8), :] = v

    def ones_sum(index, n):
        acc = None
        for d in range(-R, R + 1):
            ok = (index + d >= 0) & (index + d < n)
            term = jnp.where(ok, k[abs(d)], 0.0)
            acc = term if acc is None else acc + term
        return acc

    sum_z = ones_sum(lane + mz * BZ, nz * BZ)
    sum_y = [ones_sum(sub + (my * BY + 8 * j), ny * BY) * sum_z for j in range(TY)]
    sum_x = [ones_sum(mx * BX + i, nx * BX) for i in range(BX)]

    for c in loads[:2]:
        c.wait()
    acc = pack_init()
    total_a, total_b = zero, zero
    for j in range(TY):
        rows = pl.ds(8 * j, 8)
        for i in range(BX):
            a = a_ref[i, rows, :]
            total_a = total_a + a
            total_b = total_b + b_ref[i, rows, :]
            f[1, R + i, pl.ds(8 + 8 * j, 8), :] = jnp.ones((8, BZ), F32)
            put(0, i, j, a / (sum_x[i] * sum_y[j]), acc)
    flush(0, acc)
    total_a = jnp.broadcast_to(jnp.sum(total_a, axis=0, keepdims=True), (8, BZ))
    total_b = jnp.broadcast_to(jnp.sum(total_b, axis=0, keepdims=True), (8, BZ))
    tots[0, 0] = jnp.where(sub == 0, total_a, jnp.where(sub == 1, total_b, zero))
    pl.semaphore_wait(barrier, expected)
    start(0)
    for j in range(TY):
        face_start(0, j)

    def v_step(n):
        acc = pack_init()

        def use(i, j, ku):
            v = f[1, R + i, pl.ds(8 + 8 * j, 8), :]
            w[n, i, pl.ds(8 * j, 8), :] = v * ku
            put(1, i, j, b_ref[i, pl.ds(8 * j, 8), :] / ku, acc)

        apply(0, use, lambda j: face_start(1, j))
        flush(1, acc)
        start(1)
        sent(0)

    def u_step():
        acc = pack_init()

        def use(i, j, kv):
            put(0, i, j, a_ref[i, pl.ds(8 * j, 8), :] / kv, acc)

        apply(1, use, lambda j: face_start(0, j))
        flush(0, acc)
        start(0)
        sent(1)

    def iteration(n, carry):
        v_step(n)

        @pl.when(n == 3)
        def _():
            line("gx", 0, True)

        @pl.when(n == 4)
        def _():
            line_end("gy", 0)
            line("gz", 0, True)

        u_step()

        @pl.when(n == 3)
        def _():
            line_end("gx", 0)
            line("gy", 0, True)

        return carry

    lax.fori_loop(0, ITERS - 1, iteration, 0)
    v_step(ITERS - 1)

    line_end("gz", 0)

    def everything(row):
        v = jnp.where(sub == row, tots[0, 3], zero)
        return jnp.full((8, BZ), cells, F32) / jnp.full((8, BZ), jnp.sum(v), F32)

    alpha, beta = everything(0), everything(1)
    rows = zero
    for n in range(ITERS):
        part = zero
        for i in range(BX):
            for j in range(TY):
                at = pl.ds(8 * j, 8)
                part = part + jnp.abs(alpha * w[n, i, at, :] - beta * b_ref[i, at, :])
        part = jnp.broadcast_to(jnp.sum(part, axis=0, keepdims=True), (8, BZ))
        rows = jnp.where(sub == n, part, rows)
    tots[1, 0] = rows
    line("gx", 1, True)

    def x_copy(c, d):
        lands = 0 if d > 0 else 2 * BX
        e = 0 if d > 0 else 1
        return pltpu.make_async_remote_copy(
            src_ref=xb.at[c, pl.ds(BX, BX)], dst_ref=xb.at[c, pl.ds(lands, BX)],
            send_sem=xsend.at[c, e], recv_sem=xrecv.at[c, e],
            device_id={"gx": mx + d}, device_id_type=MESH,
        )

    def y_copy(c, d):
        i = YZ.index(d)
        _, dy, dz = d
        if dz == 0:
            ys = pl.ds(BY, 8) if dy > 0 else pl.ds(8, 8)
            yd = pl.ds(0, 8) if dy > 0 else pl.ds(BY + 8, 8)
            source, target = yb.at[c, :, ys], yb.at[c, :, yd]
        else:
            side = 0 if dz > 0 else 1
            rows = {1: pl.ds(BY - 8, 8), -1: pl.ds(0, 8), 0: pl.ds(0, BY)}[dy]
            lands = {1: pl.ds(0, 8), -1: pl.ds(BY + 8, 8), 0: pl.ds(8, BY)}[dy]
            source, target = pz.at[c, rows], zs.at[c, side, lands]
        return pltpu.make_async_remote_copy(
            src_ref=source, dst_ref=target, send_sem=ysend.at[c, i],
            recv_sem=yrecv.at[c, i], device_id=peer(d), device_id_type=MESH,
        )

    def x_start(c):
        for d in (-1, 1):
            @pl.when(conds[0][d])
            def _():
                x_copy(c, d).start()

    def x_arrived(c):
        for d in (-1, 1):
            @pl.when(conds[0][-d])
            def _():
                x_copy(c, d).wait_recv()

    def y_start(c):
        for d in YZ:
            @pl.when(has(d))
            def _():
                y_copy(c, d).start()

    def y_arrived(c):
        for d in YZ:
            @pl.when(has(neg(d)))
            def _():
                y_copy(c, d).wait_recv()

    def y_put(c, value):
        for j in range(TY):
            packed = None
            for i in range(BX):
                v = value(i, j)
                yb[c, i, pl.ds(8 + 8 * j, 8), :] = v
                moved = roll(v, 16 * i + 8)
                packed = moved if packed is None else jnp.where(
                    (lane >= 16 * i) & (lane < 16 * i + 16), moved, packed
                )
            pz[c, pl.ds(8 * j, 8), :] = packed

    def smooth_x(c, i, j):
        return symmetric(s, lambda d: xb[c, BX + i + d, pl.ds(8 * j, 8), :])

    def smooth_yz(c, put_value):
        for j in range(TY + 2):
            at = pl.ds(8 * j, 8)
            tz2[at, :] = jnp.where((lane % 16) < S, zs[c, 0, at, :], zs[c, 1, at, :])
        for j in range(TY):
            halos = symmetric(s, y_at(tz2, j))
            for i in range(BX):
                own = symmetric(s, y_at(yb.at[c, i], j))
                put_value(i, j, along_z(own, roll(halos, -(16 * i + 8)), s, [symmetric])[0])

    def at_z(i, halos):
        return roll(halos, -(8 * (i + R) + 4))

    arrived(1, SMALL)
    for j in range(TY):
        face_arrived(1, j)
    for j in range(TY + 2):
        x_tile(1, j, t, [symmetric, slope])
    x_pass_packed(1, tz, [symmetric, slope])
    for j in range(TY):
        halos = symmetric(k, y_at(tz.at[0], j))
        for i in range(BX):
            kk = symmetric(k, y_at(t.at[0, i], j))
            kvol, znum = along_z(kk, at_z(i, halos), k, [symmetric, slope])
            inverse = 1.0 / kvol
            inv[i, pl.ds(8 * j, 8), :] = inverse
            xb[2, BX + i, pl.ds(8 * j, 8), :] = znum * inverse
    x_start(2)

    halos = [slope(k, y_at(tz.at[0], j)) for j in range(TY)]

    def raw_y(i, j):
        kg = slope(k, y_at(t.at[0, i], j))
        return along_z(kg, at_z(i, halos[j]), k, [symmetric])[0] * inv[i, pl.ds(8 * j, 8), :]

    y_put(1, raw_y)
    y_start(1)

    for j in range(TY):
        halos = symmetric(k, y_at(tz.at[1], j))
        for i in range(BX):
            gk = symmetric(k, y_at(t.at[1, i], j))
            xnum = along_z(gk, at_z(i, halos), k, [symmetric])[0]
            xb[0, BX + i, pl.ds(8 * j, 8), :] = xnum * inv[i, pl.ds(8 * j, 8), :]
    x_start(0)
    sent(1)
    line_end("gx", 1)
    line("gy", 1, True)

    y_arrived(1)

    def to_x(i, j, v):
        xb[1, BX + i, pl.ds(8 * j, 8), :] = v

    smooth_yz(1, to_x)
    x_start(1)
    line_end("gy", 1)
    line("gz", 1, True)

    def to_out(c):
        def put_value(i, j, v):
            out[c, i, pl.ds(8 * j, 8), :] = v

        return put_value

    for c in (2, 0):
        x_arrived(c)
        y_put(c, functools.partial(smooth_x, c))
        y_start(c)
    y_arrived(2)
    smooth_yz(2, to_out(2))
    x_arrived(1)
    for j in range(TY):
        for i in range(BX):
            to_out(1)(i, j, smooth_x(1, i, j))
    y_arrived(0)
    smooth_yz(0, to_out(0))

    line_end("gz", 1)
    done = tots[1, 3]
    for n in range(ITERS):
        mis[n] = jnp.sum(jnp.where(sub == n, done, 0.0)) / cells
    for c in range(3):
        for d in (-1, 1):
            @pl.when(conds[0][d])
            def _():
                x_copy(c, d).wait_send()
        for d in YZ:
            @pl.when(has(d))
            def _():
                y_copy(c, d).wait_send()


def solution(mesh):
    sizes = tuple(mesh.shape[a] for a in ("gx", "gy", "gz"))
    peers = sum(sizes) - 3

    def step(source, target, kernel_half, smooth_half):
        return pl.pallas_call(
            functools.partial(kernel, sizes),
            out_shape=(
                jax.ShapeDtypeStruct((3, BX, BY, BZ), F32),
                jax.ShapeDtypeStruct((ITERS,), F32),
            ),
            in_specs=[pl.BlockSpec(memory_space=pltpu.HBM)] * 4,
            out_specs=(
                pl.BlockSpec(memory_space=pltpu.VMEM),
                pl.BlockSpec(memory_space=pltpu.SMEM),
            ),
            scratch_shapes=[
                pltpu.VMEM((BX, BY, BZ), F32),
                pltpu.VMEM((BX, BY, BZ), F32),
                pltpu.SMEM((R + 1,), F32),
                pltpu.SMEM((S + 1,), F32),
                pltpu.VMEM((2, BX + 3 * R, BY + 16, BZ), F32),
                pltpu.VMEM((2, 16, BZ), F32),
                pltpu.VMEM((2, 2, 3, 32, BZ), F32),
                pltpu.VMEM((2, BX, BY + 16, BZ), F32),
                pltpu.VMEM((2, BY + 16, BZ), F32),
                pltpu.VMEM((ITERS, BX, BY, BZ), F32),
                pltpu.VMEM((2, 4, 8, BZ), F32),
                pltpu.VMEM((2, peers, 8, BZ), F32),
                pltpu.VMEM((BX, BY, BZ), F32),
                pltpu.VMEM((3, 3 * BX, BY, BZ), F32),
                pltpu.VMEM((3, BX, BY + 16, BZ), F32),
                pltpu.VMEM((3, BY, BZ), F32),
                pltpu.VMEM((3, 2, BY + 16, BZ), F32),
                pltpu.VMEM((BY + 16, BZ), F32),
                pltpu.SemaphoreType.DMA((2, 26)),
                pltpu.SemaphoreType.DMA((2, 26)),
                pltpu.SemaphoreType.DMA((2, 2, TY)),
                pltpu.SemaphoreType.DMA((2, 2, TY)),
                pltpu.SemaphoreType.DMA((3, 2)),
                pltpu.SemaphoreType.DMA((3, 2)),
                pltpu.SemaphoreType.DMA((3, 8)),
                pltpu.SemaphoreType.DMA((3, 8)),
                pltpu.SemaphoreType.DMA((2, peers)),
                pltpu.SemaphoreType.DMA((2, peers)),
                pltpu.SemaphoreType.DMA((4,)),
            ],
            compiler_params=pltpu.CompilerParams(
                collective_id=0, has_side_effects=True, vmem_limit_bytes=67043328
            ),
        )(source, target, kernel_half, smooth_half)

    placed = P("gx", "gy", "gz")
    return jax.shard_map(
        step,
        mesh=mesh,
        in_specs=(placed, placed, P(), P()),
        out_specs=(P(None, "gx", "gy", "gz"), P()),
        check_vma=False,
    )
```

```python
import functools

import jax
import jax.numpy as jnp
from jax import lax
from jax.experimental import pallas as pl
from jax.experimental.pallas import tpu as pltpu
from jax.sharding import PartitionSpec as P

ITERS = 6
R = 4
S = 8
BX, BY, BZ = 8, 32, 128
TY = BY // 8
MESH = pl.DeviceIdType.MESH
F32 = jnp.float32

DIRS = sorted(
    [
        (dx, dy, dz)
        for dx in (-1, 0, 1)
        for dy in (-1, 0, 1)
        for dz in (-1, 0, 1)
        if (dx, dy, dz) != (0, 0, 0)
    ],
    key=lambda d: (d[1:] == (0, 0), -sum(abs(c) for c in d), -abs(d[0]), -abs(d[2]), d),
)
YZ = [d for d in DIRS if d[0] == 0]


def kernel(
    sizes,
    src_hbm, tgt_hbm, kern_hbm, smo_hbm,
    disp_hbm, mis,
    a_ref, b_ref, kern, smo, f, zp, zb, t, tz, w, tots, totb, inv, out,
    xb, yb, pz, zs, tz2,
    send, recv, xsend, xrecv, ysend, yrecv, lsend, lrecv, loc,
):
    nx, ny, nz = sizes
    cells = float(nx * ny * nz * BX * BY * BZ)
    mx, my, mz = lax.axis_index("gx"), lax.axis_index("gy"), lax.axis_index("gz")
    pos = {"gx": (mx, nx), "gy": (my, ny), "gz": (mz, nz)}
    lane = lax.broadcasted_iota(jnp.int32, (8, BZ), 1)
    sub = lax.broadcasted_iota(jnp.int32, (8, BZ), 0)
    zero = jnp.zeros((8, BZ), F32)

    loads = [
        pltpu.make_async_copy(src_hbm, a_ref, loc.at[0]),
        pltpu.make_async_copy(tgt_hbm, b_ref, loc.at[1]),
        pltpu.make_async_copy(kern_hbm, kern, loc.at[2]),
        pltpu.make_async_copy(smo_hbm, smo, loc.at[3]),
    ]
    for c in loads:
        c.start()

    def inside(m, n, d):
        if d == 0:
            return None
        return m + d < n if d > 0 else m + d >= 0

    conds = [{d: inside(m, n, d) for d in (-1, 0, 1)} for m, n in pos.values()]

    def has(d):
        c = [conds[i][d[i]] for i in range(3) if d[i]]
        return functools.reduce(jnp.logical_and, c)

    def peer(d):
        ids = {}
        for axis, step in zip(pos, d):
            if step:
                ids[axis] = pos[axis][0] + step
        return ids

    def neg(d):
        return tuple(-c for c in d)

    for p in range(2):
        for i in range(2 * R + BX):
            for j in range(TY + 2):
                f[p, i, pl.ds(8 * j, 8), :] = zero
        for q in range(2):
            for e in range(3):
                for j in range(4):
                    zb[p, q, e, j] = zero

    barrier = pltpu.get_barrier_semaphore()
    expected = 0
    for d in DIRS:
        there = has(d)
        expected = expected + jnp.where(there, 1, 0)

        @pl.when(there)
        def _():
            pl.semaphore_signal(barrier, 1, device_id=peer(d), device_id_type=MESH)

    for c in range(3):
        for i in range(BX):
            for j in range(TY):
                xb[c, i, pl.ds(8 * j, 8), :] = zero
                xb[c, 2 * BX + i, pl.ds(8 * j, 8), :] = zero
            for j in (0, TY + 1):
                yb[c, i, pl.ds(8 * j, 8), :] = zero
        for q in range(2):
            for j in range(TY + 2):
                zs[c, q, pl.ds(8 * j, 8), :] = zero

    for c in loads[2:]:
        c.wait()
    k = [kern[i] for i in range(R + 1)]
    norm = smo[0]
    tail = smo[1]
    for i in range(2, S + 1):
        tail = tail + smo[i]
    norm = jnp.full((8, BZ), norm + 2.0 * tail, F32)
    s = [jnp.full((8, BZ), smo[i], F32) / norm for i in range(S + 1)]

    def copy(p, d):
        i = DIRS.index(d)
        dx, dy, dz = d
        if dz == 0:
            xs = {1: pl.ds(BX, R), -1: pl.ds(R, R), 0: pl.ds(R, BX)}[dx]
            xd = {1: pl.ds(0, R), -1: pl.ds(R + BX, R), 0: pl.ds(R, BX)}[dx]
            ys = {1: pl.ds(BY + 8 - R, R), -1: pl.ds(8, R), 0: pl.ds(8, BY)}[dy]
            yd = {1: pl.ds(8 - R, R), -1: pl.ds(BY + 8, R), 0: pl.ds(8, BY)}[dy]
            source, target = f.at[p, xs, ys], f.at[p, xd, yd]
        else:
            side = 0 if dz > 0 else 1
            layers = {1: pl.ds(1, 1), -1: pl.ds(0, 1), 0: pl.ds(0, 2)}[dx]
            lands = {1: pl.ds(0, 1), -1: pl.ds(3, 1), 0: pl.ds(1, 2)}[dx]
            rows = {1: pl.ds(8 - R, R), -1: pl.ds(0, R), 0: pl.ds(0, 8)}[dy]
            source, target = zp.at[p, layers, rows], zb.at[p, side, 1 - dy, lands, rows]
        return pltpu.make_async_remote_copy(
            src_ref=source, dst_ref=target, send_sem=send.at[p, i],
            recv_sem=recv.at[p, i], device_id=peer(d), device_id_type=MESH,
        )

    def start(p):
        for d in DIRS:
            @pl.when(has(d))
            def _():
                copy(p, d).start()

    def sent(p):
        for d in DIRS:
            @pl.when(has(d))
            def _():
                copy(p, d).wait_send()

    def arrived(p, dirs):
        for d in dirs:
            @pl.when(has(neg(d)))
            def _():
                copy(p, d).wait_recv()

    def line(axis, q, go):
        m, n = pos[axis]
        base = {"gx": 0, "gy": nx - 1, "gz": nx + ny - 2}[axis]
        for j in range(1, n):
            c = pltpu.make_async_remote_copy(
                src_ref=tots.at[q, "xyz".index(axis[1])], dst_ref=totb.at[q, base + j - 1],
                send_sem=lsend.at[q, base + j - 1], recv_sem=lrecv.at[q, base + j - 1],
                device_id={axis: lax.rem(m + j, n)}, device_id_type=MESH,
            )
            if go:
                c.start()
            else:
                c.wait()

    def line_end(axis, q):
        line(axis, q, False)
        n = pos[axis][1]
        a = "xyz".index(axis[1])
        base = {"gx": 0, "gy": nx - 1, "gz": nx + ny - 2}[axis]
        v = tots[q, a]
        for j in range(1, n):
            v = v + totb[q, base + j - 1]
        tots[q, a + 1] = v

    def symmetric(taps, at):
        acc = taps[0] * at(0)
        for d in range(1, len(taps)):
            acc = acc + taps[d] * (at(d) + at(-d))
        return acc

    def slope(taps, at):
        acc = None
        for d in range(1, len(taps)):
            term = (float(d) * taps[d]) * (at(d) - at(-d))
            acc = term if acc is None else acc + term
        return acc

    def roll(v, by):
        by = by % BZ
        return v if by == 0 else pltpu.roll(v, by, 1)

    def along_z(own, halo, taps, passes):
        n = len(taps)
        shifted = {0: own}
        for d in range(1, n):
            shifted[d] = roll(jnp.where(lane < d, halo, own), -d)
            shifted[-d] = roll(jnp.where(lane >= BZ - d, halo, own), d)
        return [q(taps, lambda d: shifted[d]) for q in passes]

    def packed_in(p):
        left = (lane % 8) < R
        tiles = []
        for e, hs in enumerate(((TY - 1,), range(TY), (0,))):
            parts = [
                jnp.where(left, zb[p, 0, e, g], zb[p, 1, e, g])
                for g in range(4)
            ]
            for h in hs:
                moved = [roll(parts[g], 32 * (g - h)) for g in range(4)]
                tiles.append(
                    jnp.where(
                        lane < 64,
                        jnp.where(lane < 32, moved[0], moved[1]),
                        jnp.where(lane < 96, moved[2], moved[3]),
                    )
                )
        return tiles

    def x_pass(p, dst, passes):
        for j in range(TY + 2):
            rows = pl.ds(8 * j, 8)
            col = [f[p, i, rows, :] for i in range(2 * R + BX)]
            for i in range(BX):
                for n, q in enumerate(passes):
                    dst[n, i, rows, :] = q(k, lambda d: col[i + R + d])

    def x_pass_packed(p, dst, passes):
        for j, z in enumerate(packed_in(p)):
            moved = {d: roll(z, -8 * d) for d in range(-R, R + 1)}
            for n, q in enumerate(passes):
                dst[n, pl.ds(8 * j, 8), :] = q(k, lambda d: moved[d])

    def y_at(ref, j):
        return lambda d: ref[pl.ds(8 + 8 * j + d, 8), :]

    def pack_init():
        return {}

    def pack(acc, v, i, j):
        e, g = divmod(i, 4)
        at = 32 * j + 8 * g
        moved = roll(v, at + 4)
        acc[e] = moved if e not in acc else jnp.where((lane >= at) & (lane < at + 8), moved, acc[e])

    def apply(p, use):
        x_pass(p, t, [symmetric])
        x_pass_packed(p, tz, [symmetric])
        for j in range(TY):
            halos = symmetric(k, y_at(tz.at[0], j))
            for i in range(BX):
                own = symmetric(k, y_at(t.at[0, i], j))
                halo = roll(halos, -(8 * (i + R) + 4))
                use(i, j, along_z(own, halo, k, [symmetric])[0])

    def put(p, i, j, v, acc):
        f[p, R + i, pl.ds(8 + 8 * j, 8), :] = v
        pack(acc, v, i, j)

    def flush(p, acc):
        for e, v in acc.items():
            zp[p, e] = v

    def ones_sum(index, n):
        acc = None
        for d in range(-R, R + 1):
            ok = (index + d >= 0) & (index + d < n)
            term = jnp.where(ok, k[abs(d)], 0.0)
            acc = term if acc is None else acc + term
        return acc

    sum_z = ones_sum(lane + mz * BZ, nz * BZ)
    sum_y = [ones_sum(sub + (my * BY + 8 * j), ny * BY) * sum_z for j in range(TY)]
    sum_x = [ones_sum(mx * BX + i, nx * BX) for i in range(BX)]

    for c in loads[:2]:
        c.wait()
    acc = pack_init()
    total_a, total_b = zero, zero
    for j in range(TY):
        rows = pl.ds(8 * j, 8)
        for i in range(BX):
            a = a_ref[i, rows, :]
            total_a = total_a + a
            total_b = total_b + b_ref[i, rows, :]
            f[1, R + i, pl.ds(8 + 8 * j, 8), :] = jnp.ones((8, BZ), F32)
            put(0, i, j, a / (sum_x[i] * sum_y[j]), acc)
    flush(0, acc)
    total_a = jnp.broadcast_to(jnp.sum(total_a, axis=0, keepdims=True), (8, BZ))
    total_b = jnp.broadcast_to(jnp.sum(total_b, axis=0, keepdims=True), (8, BZ))
    tots[0, 0] = jnp.where(sub == 0, total_a, jnp.where(sub == 1, total_b, zero))
    pl.semaphore_wait(barrier, expected)
    start(0)

    def v_step(n):
        arrived(0, DIRS)
        acc = pack_init()

        def use(i, j, ku):
            v = f[1, R + i, pl.ds(8 + 8 * j, 8), :]
            w[n, i, pl.ds(8 * j, 8), :] = v * ku
            put(1, i, j, b_ref[i, pl.ds(8 * j, 8), :] / ku, acc)

        apply(0, use)
        flush(1, acc)
        start(1)
        sent(0)

    def u_step():
        arrived(1, DIRS)
        acc = pack_init()

        def use(i, j, kv):
            put(0, i, j, a_ref[i, pl.ds(8 * j, 8), :] / kv, acc)

        apply(1, use)
        flush(0, acc)
        start(0)
        sent(1)

    def iteration(n, carry):
        v_step(n)

        @pl.when(n == 3)
        def _():
            line("gx", 0, True)

        @pl.when(n == 4)
        def _():
            line_end("gy", 0)
            line("gz", 0, True)

        u_step()

        @pl.when(n == 3)
        def _():
            line_end("gx", 0)
            line("gy", 0, True)

        return carry

    lax.fori_loop(0, ITERS - 1, iteration, 0)
    v_step(ITERS - 1)

    line_end("gz", 0)

    def everything(row):
        v = jnp.where(sub == row, tots[0, 3], zero)
        return jnp.full((8, BZ), cells, F32) / jnp.full((8, BZ), jnp.sum(v), F32)

    alpha, beta = everything(0), everything(1)
    rows = zero
    for n in range(ITERS):
        part = zero
        for i in range(BX):
            for j in range(TY):
                at = pl.ds(8 * j, 8)
                part = part + jnp.abs(alpha * w[n, i, at, :] - beta * b_ref[i, at, :])
        part = jnp.broadcast_to(jnp.sum(part, axis=0, keepdims=True), (8, BZ))
        rows = jnp.where(sub == n, part, rows)
    tots[1, 0] = rows
    line("gx", 1, True)

    def x_copy(c, d):
        lands = 0 if d > 0 else 2 * BX
        e = 0 if d > 0 else 1
        return pltpu.make_async_remote_copy(
            src_ref=xb.at[c, pl.ds(BX, BX)], dst_ref=xb.at[c, pl.ds(lands, BX)],
            send_sem=xsend.at[c, e], recv_sem=xrecv.at[c, e],
            device_id={"gx": mx + d}, device_id_type=MESH,
        )

    def y_copy(c, d):
        i = YZ.index(d)
        _, dy, dz = d
        if dz == 0:
            ys = pl.ds(BY, 8) if dy > 0 else pl.ds(8, 8)
            yd = pl.ds(0, 8) if dy > 0 else pl.ds(BY + 8, 8)
            source, target = yb.at[c, :, ys], yb.at[c, :, yd]
        else:
            side = 0 if dz > 0 else 1
            rows = {1: pl.ds(BY - 8, 8), -1: pl.ds(0, 8), 0: pl.ds(0, BY)}[dy]
            lands = {1: pl.ds(0, 8), -1: pl.ds(BY + 8, 8), 0: pl.ds(8, BY)}[dy]
            source, target = pz.at[c, rows], zs.at[c, side, lands]
        return pltpu.make_async_remote_copy(
            src_ref=source, dst_ref=target, send_sem=ysend.at[c, i],
            recv_sem=yrecv.at[c, i], device_id=peer(d), device_id_type=MESH,
        )

    def x_start(c):
        for d in (-1, 1):
            @pl.when(conds[0][d])
            def _():
                x_copy(c, d).start()

    def x_arrived(c):
        for d in (-1, 1):
            @pl.when(conds[0][-d])
            def _():
                x_copy(c, d).wait_recv()

    def y_start(c):
        for d in YZ:
            @pl.when(has(d))
            def _():
                y_copy(c, d).start()

    def y_arrived(c):
        for d in YZ:
            @pl.when(has(neg(d)))
            def _():
                y_copy(c, d).wait_recv()

    def y_put(c, value):
        for j in range(TY):
            packed = None
            for i in range(BX):
                v = value(i, j)
                yb[c, i, pl.ds(8 + 8 * j, 8), :] = v
                moved = roll(v, 16 * i + 8)
                packed = moved if packed is None else jnp.where(
                    (lane >= 16 * i) & (lane < 16 * i + 16), moved, packed
                )
            pz[c, pl.ds(8 * j, 8), :] = packed

    def smooth_x(c, i, j):
        return symmetric(s, lambda d: xb[c, BX + i + d, pl.ds(8 * j, 8), :])

    def smooth_yz(c, put_value):
        for j in range(TY + 2):
            at = pl.ds(8 * j, 8)
            tz2[at, :] = jnp.where((lane % 16) < S, zs[c, 0, at, :], zs[c, 1, at, :])
        for j in range(TY):
            halos = symmetric(s, y_at(tz2, j))
            for i in range(BX):
                own = symmetric(s, y_at(yb.at[c, i], j))
                put_value(i, j, along_z(own, roll(halos, -(16 * i + 8)), s, [symmetric])[0])

    def at_z(i, halos):
        return roll(halos, -(8 * (i + R) + 4))

    arrived(1, DIRS)
    x_pass(1, t, [symmetric, slope])
    x_pass_packed(1, tz, [symmetric, slope])
    for j in range(TY):
        halos = symmetric(k, y_at(tz.at[0], j))
        for i in range(BX):
            kk = symmetric(k, y_at(t.at[0, i], j))
            kvol, znum = along_z(kk, at_z(i, halos), k, [symmetric, slope])
            inverse = 1.0 / kvol
            inv[i, pl.ds(8 * j, 8), :] = inverse
            xb[2, BX + i, pl.ds(8 * j, 8), :] = znum * inverse
    x_start(2)

    halos = [slope(k, y_at(tz.at[0], j)) for j in range(TY)]

    def raw_y(i, j):
        kg = slope(k, y_at(t.at[0, i], j))
        return along_z(kg, at_z(i, halos[j]), k, [symmetric])[0] * inv[i, pl.ds(8 * j, 8), :]

    y_put(1, raw_y)
    y_start(1)

    for j in range(TY):
        halos = symmetric(k, y_at(tz.at[1], j))
        for i in range(BX):
            gk = symmetric(k, y_at(t.at[1, i], j))
            xnum = along_z(gk, at_z(i, halos), k, [symmetric])[0]
            xb[0, BX + i, pl.ds(8 * j, 8), :] = xnum * inv[i, pl.ds(8 * j, 8), :]
    x_start(0)
    sent(1)
    line_end("gx", 1)
    line("gy", 1, True)

    y_arrived(1)

    def to_x(i, j, v):
        xb[1, BX + i, pl.ds(8 * j, 8), :] = v

    smooth_yz(1, to_x)
    x_start(1)
    line_end("gy", 1)
    line("gz", 1, True)

    def to_out(c):
        def put_value(i, j, v):
            out[c, i, pl.ds(8 * j, 8), :] = v

        return put_value

    for c in (2, 0):
        x_arrived(c)
        y_put(c, functools.partial(smooth_x, c))
        y_start(c)
    stores = [pltpu.make_async_copy(out.at[c], disp_hbm.at[c], loc.at[4 + c]) for c in range(3)]
    y_arrived(2)
    smooth_yz(2, to_out(2))
    stores[2].start()
    x_arrived(1)
    for j in range(TY):
        for i in range(BX):
            to_out(1)(i, j, smooth_x(1, i, j))
    stores[1].start()
    y_arrived(0)
    smooth_yz(0, to_out(0))
    stores[0].start()

    line_end("gz", 1)
    done = tots[1, 3]
    for n in range(ITERS):
        mis[n] = jnp.sum(jnp.where(sub == n, done, 0.0)) / cells
    for c in range(3):
        for d in (-1, 1):
            @pl.when(conds[0][d])
            def _():
                x_copy(c, d).wait_send()
        for d in YZ:
            @pl.when(has(d))
            def _():
                y_copy(c, d).wait_send()
        stores[c].wait()


def solution(mesh):
    sizes = tuple(mesh.shape[a] for a in ("gx", "gy", "gz"))
    peers = sum(sizes) - 3

    def step(source, target, kernel_half, smooth_half):
        return pl.pallas_call(
            functools.partial(kernel, sizes),
            out_shape=(
                jax.ShapeDtypeStruct((3, BX, BY, BZ), F32),
                jax.ShapeDtypeStruct((ITERS,), F32),
            ),
            in_specs=[pl.BlockSpec(memory_space=pltpu.HBM)] * 4,
            out_specs=(
                pl.BlockSpec(memory_space=pltpu.HBM),
                pl.BlockSpec(memory_space=pltpu.SMEM),
            ),
            scratch_shapes=[
                pltpu.VMEM((BX, BY, BZ), F32),
                pltpu.VMEM((BX, BY, BZ), F32),
                pltpu.SMEM((R + 1,), F32),
                pltpu.SMEM((S + 1,), F32),
                pltpu.VMEM((2, BX + 2 * R, BY + 16, BZ), F32),
                pltpu.VMEM((2, 2, 8, BZ), F32),
                pltpu.VMEM((2, 2, 3, 4, 8, BZ), F32),
                pltpu.VMEM((2, BX, BY + 16, BZ), F32),
                pltpu.VMEM((2, BY + 16, BZ), F32),
                pltpu.VMEM((ITERS, BX, BY, BZ), F32),
                pltpu.VMEM((2, 4, 8, BZ), F32),
                pltpu.VMEM((2, peers, 8, BZ), F32),
                pltpu.VMEM((BX, BY, BZ), F32),
                pltpu.VMEM((3, BX, BY, BZ), F32),
                pltpu.VMEM((3, 3 * BX, BY, BZ), F32),
                pltpu.VMEM((3, BX, BY + 16, BZ), F32),
                pltpu.VMEM((3, BY, BZ), F32),
                pltpu.VMEM((3, 2, BY + 16, BZ), F32),
                pltpu.VMEM((BY + 16, BZ), F32),
                pltpu.SemaphoreType.DMA((2, 26)),
                pltpu.SemaphoreType.DMA((2, 26)),
                pltpu.SemaphoreType.DMA((3, 2)),
                pltpu.SemaphoreType.DMA((3, 2)),
                pltpu.SemaphoreType.DMA((3, 8)),
                pltpu.SemaphoreType.DMA((3, 8)),
                pltpu.SemaphoreType.DMA((2, peers)),
                pltpu.SemaphoreType.DMA((2, peers)),
                pltpu.SemaphoreType.DMA((7,)),
            ],
            compiler_params=pltpu.CompilerParams(
                collective_id=0, has_side_effects=True, vmem_limit_bytes=67043328
            ),
        )(source, target, kernel_half, smooth_half)

    placed = P("gx", "gy", "gz")
    return jax.shard_map(
        step,
        mesh=mesh,
        in_specs=(placed, placed, P(), P()),
        out_specs=(P(None, "gx", "gy", "gz"), P()),
        check_vma=False,
    )
```

```python
import functools

import jax
import jax.numpy as jnp
from jax import lax
from jax.experimental import pallas as pl
from jax.experimental.pallas import tpu as pltpu
from jax.sharding import PartitionSpec as P

ITERS = 6
R = 4
S = 8
BX, BY, BZ = 8, 32, 128
TY = BY // 8
MESH = pl.DeviceIdType.MESH
F32 = jnp.float32

DIRS = sorted(
    [
        (dx, dy, dz)
        for dx in (-1, 0, 1)
        for dy in (-1, 0, 1)
        for dz in (-1, 0, 1)
        if (dx, dy, dz) != (0, 0, 0)
    ],
    key=lambda d: (d[1:] == (0, 0), -sum(abs(c) for c in d), -abs(d[0]), -abs(d[2]), d),
)
YZ = [d for d in DIRS if d[0] == 0]


def kernel(
    sizes,
    src_hbm, tgt_hbm, kern_hbm, smo_hbm,
    disp_hbm, mis,
    a_ref, b_ref, kern, smo, f, zp, zb, t, tz, w, tots, totb, inv, out,
    xb, yb, pz, zs, tz2,
    send, recv, xsend, xrecv, ysend, yrecv, lsend, lrecv, loc,
):
    nx, ny, nz = sizes
    cells = float(nx * ny * nz * BX * BY * BZ)
    mx, my, mz = lax.axis_index("gx"), lax.axis_index("gy"), lax.axis_index("gz")
    pos = {"gx": (mx, nx), "gy": (my, ny), "gz": (mz, nz)}
    lane = lax.broadcasted_iota(jnp.int32, (8, BZ), 1)
    sub = lax.broadcasted_iota(jnp.int32, (8, BZ), 0)
    zero = jnp.zeros((8, BZ), F32)

    loads = [
        pltpu.make_async_copy(src_hbm, a_ref, loc.at[0]),
        pltpu.make_async_copy(tgt_hbm, b_ref, loc.at[1]),
        pltpu.make_async_copy(kern_hbm, kern, loc.at[2]),
        pltpu.make_async_copy(smo_hbm, smo, loc.at[3]),
    ]
    for c in loads:
        c.start()

    def inside(m, n, d):
        if d == 0:
            return None
        return m + d < n if d > 0 else m + d >= 0

    conds = [{d: inside(m, n, d) for d in (-1, 0, 1)} for m, n in pos.values()]

    def has(d):
        c = [conds[i][d[i]] for i in range(3) if d[i]]
        return functools.reduce(jnp.logical_and, c)

    def peer(d):
        ids = {}
        for axis, step in zip(pos, d):
            if step:
                ids[axis] = pos[axis][0] + step
        return ids

    def neg(d):
        return tuple(-c for c in d)

    for p in range(2):
        for i in range(2 * R + BX):
            for j in range(TY + 2):
                f[p, i, pl.ds(8 * j, 8), :] = zero
        for q in range(2):
            for e in range(3):
                for j in range(4):
                    zb[p, q, e, j] = zero

    barrier = pltpu.get_barrier_semaphore()
    expected = 0
    for d in DIRS:
        there = has(d)
        expected = expected + jnp.where(there, 1, 0)

        @pl.when(there)
        def _():
            pl.semaphore_signal(barrier, 1, device_id=peer(d), device_id_type=MESH)

    for c in range(3):
        for i in range(BX):
            for j in range(TY):
                xb[c, i, pl.ds(8 * j, 8), :] = zero
                xb[c, 2 * BX + i, pl.ds(8 * j, 8), :] = zero
            for j in (0, TY + 1):
                yb[c, i, pl.ds(8 * j, 8), :] = zero
        for q in range(2):
            for j in range(TY + 2):
                zs[c, q, pl.ds(8 * j, 8), :] = zero

    for c in loads[2:]:
        c.wait()
    k = [kern[i] for i in range(R + 1)]
    norm = smo[0]
    tail = smo[1]
    for i in range(2, S + 1):
        tail = tail + smo[i]
    norm = jnp.full((8, BZ), norm + 2.0 * tail, F32)
    s = [jnp.full((8, BZ), smo[i], F32) / norm for i in range(S + 1)]

    def copy(p, d):
        i = DIRS.index(d)
        dx, dy, dz = d
        if dz == 0:
            xs = {1: pl.ds(BX, R), -1: pl.ds(R, R), 0: pl.ds(R, BX)}[dx]
            xd = {1: pl.ds(0, R), -1: pl.ds(R + BX, R), 0: pl.ds(R, BX)}[dx]
            ys = {1: pl.ds(BY + 8 - R, R), -1: pl.ds(8, R), 0: pl.ds(8, BY)}[dy]
            yd = {1: pl.ds(8 - R, R), -1: pl.ds(BY + 8, R), 0: pl.ds(8, BY)}[dy]
            source, target = f.at[p, xs, ys], f.at[p, xd, yd]
        else:
            side = 0 if dz > 0 else 1
            layers = {1: pl.ds(1, 1), -1: pl.ds(0, 1), 0: pl.ds(0, 2)}[dx]
            lands = {1: pl.ds(0, 1), -1: pl.ds(3, 1), 0: pl.ds(1, 2)}[dx]
            rows = {1: pl.ds(8 - R, R), -1: pl.ds(0, R), 0: pl.ds(0, 8)}[dy]
            source, target = zp.at[p, layers, rows], zb.at[p, side, 1 - dy, lands, rows]
        return pltpu.make_async_remote_copy(
            src_ref=source, dst_ref=target, send_sem=send.at[p, i],
            recv_sem=recv.at[p, i], device_id=peer(d), device_id_type=MESH,
        )

    def start(p):
        for d in DIRS:
            @pl.when(has(d))
            def _():
                copy(p, d).start()

    def sent(p):
        for d in DIRS:
            @pl.when(has(d))
            def _():
                copy(p, d).wait_send()

    def arrived(p, dirs):
        for d in dirs:
            @pl.when(has(neg(d)))
            def _():
                copy(p, d).wait_recv()

    def line(axis, q, go):
        m, n = pos[axis]
        base = {"gx": 0, "gy": nx - 1, "gz": nx + ny - 2}[axis]
        for j in range(1, n):
            c = pltpu.make_async_remote_copy(
                src_ref=tots.at[q, "xyz".index(axis[1])], dst_ref=totb.at[q, base + j - 1],
                send_sem=lsend.at[q, base + j - 1], recv_sem=lrecv.at[q, base + j - 1],
                device_id={axis: lax.rem(m + j, n)}, device_id_type=MESH,
            )
            if go:
                c.start()
            else:
                c.wait()

    def line_end(axis, q):
        line(axis, q, False)
        n = pos[axis][1]
        a = "xyz".index(axis[1])
        base = {"gx": 0, "gy": nx - 1, "gz": nx + ny - 2}[axis]
        v = tots[q, a]
        for j in range(1, n):
            v = v + totb[q, base + j - 1]
        tots[q, a + 1] = v

    def symmetric(taps, at):
        acc = taps[0] * at(0)
        for d in range(1, len(taps)):
            acc = acc + taps[d] * (at(d) + at(-d))
        return acc

    def slope(taps, at):
        acc = None
        for d in range(1, len(taps)):
            term = (float(d) * taps[d]) * (at(d) - at(-d))
            acc = term if acc is None else acc + term
        return acc

    def roll(v, by):
        by = by % BZ
        return v if by == 0 else pltpu.roll(v, by, 1)

    def along_z(own, halo, taps, passes):
        n = len(taps)
        shifted = {0: own}
        for d in range(1, n):
            shifted[d] = roll(jnp.where(lane < d, halo, own), -d)
            shifted[-d] = roll(jnp.where(lane >= BZ - d, halo, own), d)
        return [q(taps, lambda d: shifted[d]) for q in passes]

    def packed_in(p):
        left = (lane % 8) < R
        tiles = []
        for e, hs in enumerate(((TY - 1,), range(TY), (0,))):
            parts = [
                jnp.where(left, zb[p, 0, e, g], zb[p, 1, e, g])
                for g in range(4)
            ]
            for h in hs:
                moved = [roll(parts[g], 32 * (g - h)) for g in range(4)]
                tiles.append(
                    jnp.where(
                        lane < 64,
                        jnp.where(lane < 32, moved[0], moved[1]),
                        jnp.where(lane < 96, moved[2], moved[3]),
                    )
                )
        return tiles

    def x_pass(p, dst, passes):
        for j in range(TY + 1):
            rows = pl.ds(8 * j, 8)
            col = [f[p, i, rows, :] for i in range(2 * R + BX)]
            if j == 0:
                last = pl.ds(8 * (TY + 1), 8)
                col = [jnp.where(sub < R, f[p, i, last, :], v) for i, v in enumerate(col)]
            for i in range(BX):
                for n, q in enumerate(passes):
                    v = q(k, lambda d: col[i + R + d])
                    dst[n, i, rows, :] = v
                    if j == 0:
                        dst[n, i, last, :] = v

    def x_pass_packed(p, dst, passes):
        tiles = packed_in(p)
        tiles[0] = jnp.where(sub < R, tiles.pop(), tiles[0])
        for j, z in enumerate(tiles):
            moved = {d: roll(z, -8 * d) for d in range(-R, R + 1)}
            for n, q in enumerate(passes):
                v = q(k, lambda d: moved[d])
                dst[n, pl.ds(8 * j, 8), :] = v
                if j == 0:
                    dst[n, pl.ds(8 * (TY + 1), 8), :] = v

    def y_at(ref, j):
        return lambda d: ref[pl.ds(8 + 8 * j + d, 8), :]

    def pack_init():
        return {}

    def pack(acc, v, i, j):
        e, g = divmod(i, 4)
        at = 32 * j + 8 * g
        moved = roll(v, at + 4)
        acc[e] = moved if e not in acc else jnp.where((lane >= at) & (lane < at + 8), moved, acc[e])

    def apply(p, use):
        x_pass(p, t, [symmetric])
        x_pass_packed(p, tz, [symmetric])
        for j in range(TY):
            halos = symmetric(k, y_at(tz.at[0], j))
            for i in range(BX):
                own = symmetric(k, y_at(t.at[0, i], j))
                halo = roll(halos, -(8 * (i + R) + 4))
                use(i, j, along_z(own, halo, k, [symmetric])[0])

    def put(p, i, j, v, acc):
        f[p, R + i, pl.ds(8 + 8 * j, 8), :] = v
        pack(acc, v, i, j)

    def flush(p, acc):
        for e, v in acc.items():
            zp[p, e] = v

    def ones_sum(index, n):
        acc = None
        for d in range(-R, R + 1):
            ok = (index + d >= 0) & (index + d < n)
            term = jnp.where(ok, k[abs(d)], 0.0)
            acc = term if acc is None else acc + term
        return acc

    sum_z = ones_sum(lane + mz * BZ, nz * BZ)
    sum_y = [ones_sum(sub + (my * BY + 8 * j), ny * BY) * sum_z for j in range(TY)]
    sum_x = [ones_sum(mx * BX + i, nx * BX) for i in range(BX)]

    for c in loads[:2]:
        c.wait()
    acc = pack_init()
    total_a, total_b = zero, zero
    for j in range(TY):
        rows = pl.ds(8 * j, 8)
        for i in range(BX):
            a = a_ref[i, rows, :]
            total_a = total_a + a
            total_b = total_b + b_ref[i, rows, :]
            f[1, R + i, pl.ds(8 + 8 * j, 8), :] = jnp.ones((8, BZ), F32)
            put(0, i, j, a / (sum_x[i] * sum_y[j]), acc)
    flush(0, acc)
    total_a = jnp.broadcast_to(jnp.sum(total_a, axis=0, keepdims=True), (8, BZ))
    total_b = jnp.broadcast_to(jnp.sum(total_b, axis=0, keepdims=True), (8, BZ))
    tots[0, 0] = jnp.where(sub == 0, total_a, jnp.where(sub == 1, total_b, zero))
    pl.semaphore_wait(barrier, expected)
    start(0)

    def v_step(n):
        arrived(0, DIRS)
        acc = pack_init()

        def use(i, j, ku):
            v = f[1, R + i, pl.ds(8 + 8 * j, 8), :]
            w[n, i, pl.ds(8 * j, 8), :] = v * ku
            put(1, i, j, b_ref[i, pl.ds(8 * j, 8), :] / ku, acc)

        apply(0, use)
        flush(1, acc)
        start(1)
        sent(0)

    def u_step():
        arrived(1, DIRS)
        acc = pack_init()

        def use(i, j, kv):
            put(0, i, j, a_ref[i, pl.ds(8 * j, 8), :] / kv, acc)

        apply(1, use)
        flush(0, acc)
        start(0)
        sent(1)

    def iteration(n, carry):
        v_step(n)

        @pl.when(n == 3)
        def _():
            line("gx", 0, True)

        @pl.when(n == 4)
        def _():
            line_end("gy", 0)
            line("gz", 0, True)

        u_step()

        @pl.when(n == 3)
        def _():
            line_end("gx", 0)
            line("gy", 0, True)

        return carry

    lax.fori_loop(0, ITERS - 1, iteration, 0)
    v_step(ITERS - 1)

    line_end("gz", 0)

    def everything(row):
        v = jnp.where(sub == row, tots[0, 3], zero)
        return jnp.full((8, BZ), cells, F32) / jnp.full((8, BZ), jnp.sum(v), F32)

    alpha, beta = everything(0), everything(1)
    rows = zero
    for n in range(ITERS):
        part = zero
        for i in range(BX):
            for j in range(TY):
                at = pl.ds(8 * j, 8)
                part = part + jnp.abs(alpha * w[n, i, at, :] - beta * b_ref[i, at, :])
        part = jnp.broadcast_to(jnp.sum(part, axis=0, keepdims=True), (8, BZ))
        rows = jnp.where(sub == n, part, rows)
    tots[1, 0] = rows
    line("gx", 1, True)

    def x_copy(c, d):
        lands = 0 if d > 0 else 2 * BX
        e = 0 if d > 0 else 1
        return pltpu.make_async_remote_copy(
            src_ref=xb.at[c, pl.ds(BX, BX)], dst_ref=xb.at[c, pl.ds(lands, BX)],
            send_sem=xsend.at[c, e], recv_sem=xrecv.at[c, e],
            device_id={"gx": mx + d}, device_id_type=MESH,
        )

    def y_copy(c, d):
        i = YZ.index(d)
        _, dy, dz = d
        if dz == 0:
            ys = pl.ds(BY, 8) if dy > 0 else pl.ds(8, 8)
            yd = pl.ds(0, 8) if dy > 0 else pl.ds(BY + 8, 8)
            source, target = yb.at[c, :, ys], yb.at[c, :, yd]
        else:
            side = 0 if dz > 0 else 1
            rows = {1: pl.ds(BY - 8, 8), -1: pl.ds(0, 8), 0: pl.ds(0, BY)}[dy]
            lands = {1: pl.ds(0, 8), -1: pl.ds(BY + 8, 8), 0: pl.ds(8, BY)}[dy]
            source, target = pz.at[c, rows], zs.at[c, side, lands]
        return pltpu.make_async_remote_copy(
            src_ref=source, dst_ref=target, send_sem=ysend.at[c, i],
            recv_sem=yrecv.at[c, i], device_id=peer(d), device_id_type=MESH,
        )

    def x_start(c):
        for d in (-1, 1):
            @pl.when(conds[0][d])
            def _():
                x_copy(c, d).start()

    def x_arrived(c):
        for d in (-1, 1):
            @pl.when(conds[0][-d])
            def _():
                x_copy(c, d).wait_recv()

    def y_start(c):
        for d in YZ:
            @pl.when(has(d))
            def _():
                y_copy(c, d).start()

    def y_arrived(c):
        for d in YZ:
            @pl.when(has(neg(d)))
            def _():
                y_copy(c, d).wait_recv()

    def y_put(c, value):
        for j in range(TY):
            packed = None
            for i in range(BX):
                v = value(i, j)
                yb[c, i, pl.ds(8 + 8 * j, 8), :] = v
                moved = roll(v, 16 * i + 8)
                packed = moved if packed is None else jnp.where(
                    (lane >= 16 * i) & (lane < 16 * i + 16), moved, packed
                )
            pz[c, pl.ds(8 * j, 8), :] = packed

    def smooth_x(c, i, j):
        return symmetric(s, lambda d: xb[c, BX + i + d, pl.ds(8 * j, 8), :])

    def smooth_yz(c, put_value):
        for j in range(TY + 2):
            at = pl.ds(8 * j, 8)
            tz2[at, :] = jnp.where((lane % 16) < S, zs[c, 0, at, :], zs[c, 1, at, :])
        for j in range(TY):
            halos = symmetric(s, y_at(tz2, j))
            for i in range(BX):
                own = symmetric(s, y_at(yb.at[c, i], j))
                put_value(i, j, along_z(own, roll(halos, -(16 * i + 8)), s, [symmetric])[0])

    def at_z(i, halos):
        return roll(halos, -(8 * (i + R) + 4))

    arrived(1, DIRS)
    x_pass(1, t, [symmetric, slope])
    x_pass_packed(1, tz, [symmetric, slope])
    for j in range(TY):
        halos = symmetric(k, y_at(tz.at[0], j))
        for i in range(BX):
            kk = symmetric(k, y_at(t.at[0, i], j))
            kvol, znum = along_z(kk, at_z(i, halos), k, [symmetric, slope])
            inverse = 1.0 / kvol
            inv[i, pl.ds(8 * j, 8), :] = inverse
            xb[2, BX + i, pl.ds(8 * j, 8), :] = znum * inverse
    x_start(2)

    halos = [slope(k, y_at(tz.at[0], j)) for j in range(TY)]

    def raw_y(i, j):
        kg = slope(k, y_at(t.at[0, i], j))
        return along_z(kg, at_z(i, halos[j]), k, [symmetric])[0] * inv[i, pl.ds(8 * j, 8), :]

    y_put(1, raw_y)
    y_start(1)

    for j in range(TY):
        halos = symmetric(k, y_at(tz.at[1], j))
        for i in range(BX):
            gk = symmetric(k, y_at(t.at[1, i], j))
            xnum = along_z(gk, at_z(i, halos), k, [symmetric])[0]
            xb[0, BX + i, pl.ds(8 * j, 8), :] = xnum * inv[i, pl.ds(8 * j, 8), :]
    x_start(0)
    sent(1)
    line_end("gx", 1)
    line("gy", 1, True)

    y_arrived(1)

    def to_x(i, j, v):
        xb[1, BX + i, pl.ds(8 * j, 8), :] = v

    smooth_yz(1, to_x)
    x_start(1)
    line_end("gy", 1)
    line("gz", 1, True)

    def to_out(c):
        def put_value(i, j, v):
            out[c, i, pl.ds(8 * j, 8), :] = v

        return put_value

    for c in (2, 0):
        x_arrived(c)
        y_put(c, functools.partial(smooth_x, c))
        y_start(c)
    stores = [pltpu.make_async_copy(out.at[c], disp_hbm.at[c], loc.at[4 + c]) for c in range(3)]
    y_arrived(2)
    smooth_yz(2, to_out(2))
    stores[2].start()
    x_arrived(1)
    for j in range(TY):
        for i in range(BX):
            to_out(1)(i, j, smooth_x(1, i, j))
    stores[1].start()
    y_arrived(0)
    smooth_yz(0, to_out(0))
    stores[0].start()

    line_end("gz", 1)
    done = tots[1, 3]
    for n in range(ITERS):
        mis[n] = jnp.sum(jnp.where(sub == n, done, 0.0)) / cells
    for c in range(3):
        for d in (-1, 1):
            @pl.when(conds[0][d])
            def _():
                x_copy(c, d).wait_send()
        for d in YZ:
            @pl.when(has(d))
            def _():
                y_copy(c, d).wait_send()
        stores[c].wait()


def solution(mesh):
    sizes = tuple(mesh.shape[a] for a in ("gx", "gy", "gz"))
    peers = sum(sizes) - 3

    def step(source, target, kernel_half, smooth_half):
        return pl.pallas_call(
            functools.partial(kernel, sizes),
            out_shape=(
                jax.ShapeDtypeStruct((3, BX, BY, BZ), F32),
                jax.ShapeDtypeStruct((ITERS,), F32),
            ),
            in_specs=[pl.BlockSpec(memory_space=pltpu.HBM)] * 4,
            out_specs=(
                pl.BlockSpec(memory_space=pltpu.HBM),
                pl.BlockSpec(memory_space=pltpu.SMEM),
            ),
            scratch_shapes=[
                pltpu.VMEM((BX, BY, BZ), F32),
                pltpu.VMEM((BX, BY, BZ), F32),
                pltpu.SMEM((R + 1,), F32),
                pltpu.SMEM((S + 1,), F32),
                pltpu.VMEM((2, BX + 2 * R, BY + 16, BZ), F32),
                pltpu.VMEM((2, 2, 8, BZ), F32),
                pltpu.VMEM((2, 2, 3, 4, 8, BZ), F32),
                pltpu.VMEM((2, BX, BY + 16, BZ), F32),
                pltpu.VMEM((2, BY + 16, BZ), F32),
                pltpu.VMEM((ITERS, BX, BY, BZ), F32),
                pltpu.VMEM((2, 4, 8, BZ), F32),
                pltpu.VMEM((2, peers, 8, BZ), F32),
                pltpu.VMEM((BX, BY, BZ), F32),
                pltpu.VMEM((3, BX, BY, BZ), F32),
                pltpu.VMEM((3, 3 * BX, BY, BZ), F32),
                pltpu.VMEM((3, BX, BY + 16, BZ), F32),
                pltpu.VMEM((3, BY, BZ), F32),
                pltpu.VMEM((3, 2, BY + 16, BZ), F32),
                pltpu.VMEM((BY + 16, BZ), F32),
                pltpu.SemaphoreType.DMA((2, 26)),
                pltpu.SemaphoreType.DMA((2, 26)),
                pltpu.SemaphoreType.DMA((3, 2)),
                pltpu.SemaphoreType.DMA((3, 2)),
                pltpu.SemaphoreType.DMA((3, 8)),
                pltpu.SemaphoreType.DMA((3, 8)),
                pltpu.SemaphoreType.DMA((2, peers)),
                pltpu.SemaphoreType.DMA((2, peers)),
                pltpu.SemaphoreType.DMA((7,)),
            ],
            compiler_params=pltpu.CompilerParams(
                collective_id=0, has_side_effects=True, vmem_limit_bytes=67043328
            ),
        )(source, target, kernel_half, smooth_half)

    placed = P("gx", "gy", "gz")
    return jax.shard_map(
        step,
        mesh=mesh,
        in_specs=(placed, placed, P(), P()),
        out_specs=(P(None, "gx", "gy", "gz"), P()),
        check_vma=False,
    )
```
